512 devices in a mesh: nodes: 128 (over z_hi, y, x, core), heads: 4 (over z_lo).
Axes of the slice: x: 4, y: 4, z: 16 (z_hi: 4, z_lo: 4; z = z_hi * 4 + z_lo), core: 2. Of those that a mesh axis runs over, the one named last changes fastest.
Arguments:
- grid_state: bfloat16 [131072, 1024], P('nodes', 'heads'), may hold values from -6 to 6
- mesh_state: bfloat16 [32768, 1024], P('nodes', 'heads'), may hold values from -6 to 6
- encoder_query: bfloat16 [1024, 512], P('nodes', 'heads'), may hold values from -0.1875 to 0.1875
- encoder_key: bfloat16 [1024, 512], P('nodes', 'heads'), may hold values from -0.1875 to 0.1875
- encoder_value: bfloat16 [1024, 512], P('nodes', 'heads'), may hold values from -0.1875 to 0.1875
- encoder_output: bfloat16 [512, 1024], P('heads', 'nodes'), may hold values from -0.25 to 0.25
- window_query: bfloat16 [1024, 512], P('nodes', 'heads'), may hold values from -0.1875 to 0.1875
- window_key: bfloat16 [1024, 512], P('nodes', 'heads'), may hold values from -0.1875 to 0.1875
- window_value: bfloat16 [1024, 512], P('nodes', 'heads'), may hold values from -0.1875 to 0.1875
- window_output: bfloat16 [512, 1024], P('heads', 'nodes'), may hold values from -0.25 to 0.25
- expand_weight: bfloat16 [1024, 2048], P('nodes', 'heads'), may hold values from -0.1875 to 0.1875
- shrink_weight: bfloat16 [2048, 1024], P('heads', 'nodes'), may hold values from -0.125 to 0.125
- decoder_query: bfloat16 [1024, 512], P('nodes', 'heads'), may hold values from -0.1875 to 0.1875
- decoder_key: bfloat16 [1024, 512], P('nodes', 'heads'), may hold values from -0.1875 to 0.1875
- decoder_value: bfloat16 [1024, 512], P('nodes', 'heads'), may hold values from -0.1875 to 0.1875
- decoder_output: bfloat16 [512, 1024], P('heads', 'nodes'), may hold values from -0.25 to 0.25
- encoder_blocks: int32 [256, 8], P('nodes'), may hold values from 0 to 1023, as said below
- encoder_count: int32 [256], P('nodes'), may hold values from 2 to 8, as said below
- window_offsets: int32 [256, 4], P('nodes'), may hold values from -2 to 2, as said below
- decoder_blocks: int32 [1024, 3], P('nodes'), may hold values from 0 to 255, as said below
- decoder_count: int32 [1024], P('nodes'), may hold values from 1 to 3, as said below
Outputs:
- grid_out: bfloat16 [131072, 1024], P('nodes', 'heads')
- mesh_out: bfloat16 [32768, 1024], P('nodes', 'heads')
The draws below stay inside these ranges and needn't reach their ends.
Inputs may be any that keep to these rules, and one draw needn't show every extreme that they name: `encoder_blocks`: row m names 8 different grid blocks; each lies among the grid blocks of the index of nodes that holds mesh block m, or in the nearer half of the grid blocks of the index on either side. The first encoder_count[m] slots of row m are live; every mesh block held by the first or last eighth of the indices of nodes has all 8 slots live. `window_offsets`: each row holds 4 different offsets, the first of them 0. `decoder_blocks`: row g names 3 different mesh blocks; each lies among the mesh blocks of the index of nodes that holds grid block g, or is the one block next to them on either side. The first decoder_count[g] slots of row g are live; every grid block of the first index of nodes has all 3 slots live.
All inputs are finite; a program needn't handle non-finite values.
Results may differ from the reference program's by a relative error of at most 0.012.
Values may be sent and summed in bfloat16 or wider, within the bound.
No kernel may reach another device: no remote copies, remote signals or barrier semaphores. Data moves between devices by JAX's collectives and lax.ppermute only.
A program may use at most 64 MiB of HBM per device.

```python
import jax
import jax.numpy as jnp
from jax import lax

D = 1024
HEADS = 8
HEAD_DIM = 64
FF = 2048
TILE = 128
ENC_SLOTS = 8
DEC_SLOTS = 3
WIN = 4
REACH = 2
GRID_DEV = 1024
MESH_DEV = 256
GRID = 131072
MESH = 32768


def distinct_pick(subkey, candidates, in_range, needed):
    column_count = candidates.shape[1]
    column_index = jnp.arange(column_count, dtype=jnp.int32)[None, :]
    random_part = jax.random.randint(subkey, candidates.shape, 0, 1 << 20)
    ranking = random_part * column_count + column_index
    ranking = jnp.where(in_range, ranking, -1 - column_index)
    _, chosen = lax.top_k(ranking, needed)
    return jnp.take_along_axis(candidates, chosen, axis=1).astype(jnp.int32)


def draw_encoder_blocks(key, part):
    grid_tiles = GRID_DEV // TILE
    mesh_tiles = MESH_DEV // TILE
    owner_index = jnp.arange(MESH // TILE, dtype=jnp.int32) // mesh_tiles
    first_tile = owner_index * grid_tiles - grid_tiles // 2
    candidates = first_tile[:, None] + jnp.arange(2 * grid_tiles, dtype=jnp.int32)[None, :]
    in_range = (candidates >= 0) & (candidates < GRID // TILE)
    return distinct_pick(jax.random.fold_in(key, 11), candidates, in_range, ENC_SLOTS)


def draw_encoder_count(key, part):
    devices = MESH // MESH_DEV
    owner_index = jnp.arange(MESH // TILE, dtype=jnp.int32) // (MESH_DEV // TILE)
    live_count = jax.random.randint(jax.random.fold_in(key, 12), (MESH // TILE,), 2, ENC_SLOTS + 1)
    crowded = (owner_index * 8 < devices) | (owner_index * 8 >= 7 * devices)
    return jnp.where(crowded, ENC_SLOTS, live_count).astype(jnp.int32)


def draw_window_offsets(key, part):
    tile_count = MESH // TILE
    others = jnp.concatenate([jnp.arange(-REACH, 0, dtype=jnp.int32), jnp.arange(1, REACH + 1, dtype=jnp.int32)])
    candidates = jnp.broadcast_to(others[None, :], (tile_count, 2 * REACH))
    in_range = jnp.ones((tile_count, 2 * REACH), dtype=bool)
    picked = distinct_pick(jax.random.fold_in(key, 13), candidates, in_range, WIN - 1)
    return jnp.concatenate([jnp.zeros((tile_count, 1), jnp.int32), picked], axis=1)


def draw_decoder_blocks(key, part):
    grid_tiles = GRID_DEV // TILE
    mesh_tiles = MESH_DEV // TILE
    owner_index = jnp.arange(GRID // TILE, dtype=jnp.int32) // grid_tiles
    first_tile = owner_index * mesh_tiles - 1
    candidates = first_tile[:, None] + jnp.arange(mesh_tiles + 2, dtype=jnp.int32)[None, :]
    in_range = (candidates >= 0) & (candidates < MESH // TILE)
    return distinct_pick(jax.random.fold_in(key, 14), candidates, in_range, DEC_SLOTS)


def draw_decoder_count(key, part):
    owner_index = jnp.arange(GRID // TILE, dtype=jnp.int32) // (GRID_DEV // TILE)
    live_count = jax.random.randint(jax.random.fold_in(key, 15), (GRID // TILE,), 1, DEC_SLOTS + 1)
    return jnp.where(owner_index == 0, DEC_SLOTS, live_count).astype(jnp.int32)


def level_of(own_key, shape, pieces, least, largest):
    factor_of, own = 1.0, jax.random.fold_in(own_key, 6)
    for position, parts in pieces:
        heights = jnp.exp(jax.random.uniform(jax.random.fold_in(own, position), (parts,), jnp.float32, least / len(pieces), largest / len(pieces)))
        factor_of = factor_of * jnp.repeat(heights, shape[position] // parts).reshape([-1 if axis == position else 1 for axis in range(len(shape))])
    return factor_of


def scatter_about(key, dims, width, limit, cuts=(), kind=jnp.bfloat16):
    result = width * jax.random.normal(key, dims, jnp.float32)
    if cuts:
        result = result * level_of(key, dims, cuts, -0.22, 0.18)
    return jnp.clip(result, -limit, limit).astype(kind)


def setup_inputs(seed: int = 0) -> dict:
    seeds = jax.random.split(jax.random.key(seed), 22)
    grid_state = scatter_about(seeds[0], (GRID, D), 1.0, 6.0, ((0, 128), (1, 4)))
    mesh_state = scatter_about(seeds[1], (MESH, D), 1.0, 6.0, ((0, 128), (1, 4)))
    encoder_query = scatter_about(seeds[2], (D, HEADS * HEAD_DIM), D ** -0.5, 0.1875, ((0, 128), (1, 4)))
    encoder_key = scatter_about(seeds[3], (D, HEADS * HEAD_DIM), D ** -0.5, 0.1875, ((0, 128), (1, 4)))
    encoder_value = scatter_about(seeds[4], (D, HEADS * HEAD_DIM), D ** -0.5, 0.1875, ((0, 128), (1, 4)))
    encoder_output = scatter_about(seeds[5], (HEADS * HEAD_DIM, D), (HEADS * HEAD_DIM) ** -0.5, 0.25, ((0, 4), (1, 128)))
    window_query = scatter_about(seeds[6], (D, HEADS * HEAD_DIM), D ** -0.5, 0.1875, ((0, 128), (1, 4)))
    window_key = scatter_about(seeds[7], (D, HEADS * HEAD_DIM), D ** -0.5, 0.1875, ((0, 128), (1, 4)))
    window_value = scatter_about(seeds[8], (D, HEADS * HEAD_DIM), D ** -0.5, 0.1875, ((0, 128), (1, 4)))
    window_output = scatter_about(seeds[9], (HEADS * HEAD_DIM, D), (HEADS * HEAD_DIM) ** -0.5, 0.25, ((0, 4), (1, 128)))
    expand_weight = scatter_about(seeds[10], (D, FF), D ** -0.5, 0.1875, ((0, 128), (1, 4)))
    shrink_weight = scatter_about(seeds[11], (FF, D), FF ** -0.5, 0.125, ((0, 4), (1, 128)))
    decoder_query = scatter_about(seeds[12], (D, HEADS * HEAD_DIM), D ** -0.5, 0.1875, ((0, 128), (1, 4)))
    decoder_key = scatter_about(seeds[13], (D, HEADS * HEAD_DIM), D ** -0.5, 0.1875, ((0, 128), (1, 4)))
    decoder_value = scatter_about(seeds[14], (D, HEADS * HEAD_DIM), D ** -0.5, 0.1875, ((0, 128), (1, 4)))
    decoder_output = scatter_about(seeds[15], (HEADS * HEAD_DIM, D), (HEADS * HEAD_DIM) ** -0.5, 0.25, ((0, 4), (1, 128)))
    encoder_blocks = draw_encoder_blocks(jax.random.fold_in(seeds[21], 71), 0)
    encoder_count = draw_encoder_count(jax.random.fold_in(seeds[21], 71), 0)
    window_offsets = draw_window_offsets(jax.random.fold_in(seeds[21], 71), 0)
    decoder_blocks = draw_decoder_blocks(jax.random.fold_in(seeds[21], 71), 0)
    decoder_count = draw_decoder_count(jax.random.fold_in(seeds[21], 71), 0)
    return {"grid_state": grid_state, "mesh_state": mesh_state, "encoder_query": encoder_query, "encoder_key": encoder_key, "encoder_value": encoder_value, "encoder_output": encoder_output, "window_query": window_query, "window_key": window_key, "window_value": window_value, "window_output": window_output, "expand_weight": expand_weight, "shrink_weight": shrink_weight, "decoder_query": decoder_query, "decoder_key": decoder_key, "decoder_value": decoder_value, "decoder_output": decoder_output, "encoder_blocks": encoder_blocks, "encoder_count": encoder_count, "window_offsets": window_offsets, "decoder_blocks": decoder_blocks, "decoder_count": decoder_count}


EPSILON = 1e-05

def normalize(values):
    values = values.astype(jnp.float32)
    average = lax.optimization_barrier(jnp.mean(values, axis=-1, keepdims=True))
    centred = values - average
    spread = lax.optimization_barrier(jnp.mean(centred * centred, axis=-1, keepdims=True))
    return (centred * lax.rsqrt(spread + EPSILON)).astype(jnp.bfloat16)

def project(source, weight, scaling):
    return (jnp.dot(source, weight, preferred_element_type=jnp.float32) * scaling).astype(jnp.bfloat16)

def residual(base, mixture, weight):
    update = jnp.dot(mixture, weight, preferred_element_type=jnp.float32)
    return (base.astype(jnp.float32) + update).astype(jnp.bfloat16)

def attend(queries, key_rows, value_rows, key_mask):
    head_count = queries.shape[1] // HEAD_DIM
    split_query = queries.astype(jnp.float32).reshape(queries.shape[0], head_count, HEAD_DIM)
    split_key = key_rows.astype(jnp.float32).reshape(key_rows.shape[0], head_count, HEAD_DIM)
    split_value = value_rows.astype(jnp.float32).reshape(value_rows.shape[0], head_count, HEAD_DIM)
    scores = jnp.einsum('qhd,khd->hqk', split_query, split_key)
    scores = jnp.where(key_mask[None, None, :], scores, -1e+30)
    highest = lax.optimization_barrier(jnp.max(scores, axis=-1, keepdims=True))
    weights = jnp.exp(scores - highest)
    weights = (weights / lax.optimization_barrier(jnp.sum(weights, axis=-1, keepdims=True))).astype(jnp.bfloat16)
    weights = lax.optimization_barrier(weights).astype(jnp.float32)
    mixture = jnp.einsum('hqk,khd->qhd', weights, split_value)
    return mixture.reshape(queries.shape).astype(jnp.bfloat16)

def reference(grid_state, mesh_state, encoder_query, encoder_key, encoder_value, encoder_output, window_query, window_key, window_value, window_output, expand_weight, shrink_weight, decoder_query, decoder_key, decoder_value, decoder_output, encoder_blocks, encoder_count, window_offsets, decoder_blocks, decoder_count):
    scaling = HEAD_DIM ** (-0.5)
    features = HEADS * HEAD_DIM
    grid_tiles = GRID // TILE
    mesh_tiles = MESH // TILE
    grid_norm = normalize(grid_state)
    grid_keys = project(grid_norm, encoder_key, 1.0).reshape(grid_tiles, TILE, features)
    grid_values = project(grid_norm, encoder_value, 1.0).reshape(grid_tiles, TILE, features)
    grid_queries = project(grid_norm, decoder_query, scaling)
    mesh_queries = project(normalize(mesh_state), encoder_query, scaling)
    enc_slots = jnp.arange(ENC_SLOTS, dtype=jnp.int32)

    def encode(arguments):
        queries, chosen, live_count = arguments
        key_mask = jnp.repeat(enc_slots < live_count, TILE)
        key_rows = grid_keys[chosen].reshape(ENC_SLOTS * TILE, features)
        value_rows = grid_values[chosen].reshape(ENC_SLOTS * TILE, features)
        return attend(queries, key_rows, value_rows, key_mask)
    encoded = lax.map(encode, (mesh_queries.reshape(mesh_tiles, TILE, features), encoder_blocks, encoder_count))
    mesh_one = residual(mesh_state, encoded.reshape(MESH, features), encoder_output)
    norm_one = normalize(mesh_one)
    window_queries = project(norm_one, window_query, scaling)
    window_keys = project(norm_one, window_key, 1.0).reshape(mesh_tiles, TILE, features)
    window_values = project(norm_one, window_value, 1.0).reshape(mesh_tiles, TILE, features)

    def window(arguments):
        queries, tile_index, offsets = arguments
        reached = tile_index + offsets
        key_mask = jnp.repeat((reached >= 0) & (reached < mesh_tiles), TILE)
        chosen = jnp.clip(reached, 0, mesh_tiles - 1)
        key_rows = window_keys[chosen].reshape(WIN * TILE, features)
        value_rows = window_values[chosen].reshape(WIN * TILE, features)
        return attend(queries, key_rows, value_rows, key_mask)
    tile_numbers = jnp.arange(mesh_tiles, dtype=jnp.int32)
    windowed = lax.map(window, (window_queries.reshape(mesh_tiles, TILE, features), tile_numbers, window_offsets))
    mesh_two = residual(mesh_one, windowed.reshape(MESH, features), window_output)
    hidden = jax.nn.gelu(jnp.dot(normalize(mesh_two), expand_weight, preferred_element_type=jnp.float32), approximate=False).astype(jnp.bfloat16)
    mesh_three = residual(mesh_two, hidden, shrink_weight)
    norm_three = normalize(mesh_three)
    mesh_keys = project(norm_three, decoder_key, 1.0).reshape(mesh_tiles, TILE, features)
    mesh_values = project(norm_three, decoder_value, 1.0).reshape(mesh_tiles, TILE, features)
    dec_slots = jnp.arange(DEC_SLOTS, dtype=jnp.int32)

    def decode(arguments):
        queries, chosen, live_count = arguments
        key_mask = jnp.repeat(dec_slots < live_count, TILE)
        key_rows = mesh_keys[chosen].reshape(DEC_SLOTS * TILE, features)
        value_rows = mesh_values[chosen].reshape(DEC_SLOTS * TILE, features)
        return attend(queries, key_rows, value_rows, key_mask)
    decoded = lax.map(decode, (grid_queries.reshape(grid_tiles, TILE, features), decoder_blocks, decoder_count))
    grid_out = residual(grid_state, decoded.reshape(GRID, features), decoder_output)
    return (grid_out, mesh_three)
```

```python
import functools

import jax
import jax.numpy as jnp
from jax import lax
from jax.experimental import pallas as pl
from jax.experimental.pallas import tpu as pltpu
from jax.sharding import Mesh
from jax.sharding import PartitionSpec as P

HEAD_DIM = 64
TILE = 128
PAIR = 2 * HEAD_DIM
D = 1024
SCALE = HEAD_DIM ** (-0.5)
EPSILON = 1e-05
NODES = ("zh", "y", "x", "core")
F32 = jnp.float32
BF16 = jnp.bfloat16


def in_vmem():
    return pl.BlockSpec(memory_space=pltpu.VMEM)


def in_smem():
    return pl.BlockSpec(memory_space=pltpu.SMEM)


def in_any():
    return pl.BlockSpec(memory_space=pltpu.HBM)


def call(kernel, name, outs, specs, scratch=(), flops=1 << 28, room=12):
    return pl.pallas_call(
        kernel,
        name=name,
        out_shape=tuple(jax.ShapeDtypeStruct(shape, BF16) for shape in outs),
        in_specs=list(specs),
        out_specs=tuple(in_vmem() for _ in outs),
        scratch_shapes=list(scratch),
        compiler_params=pltpu.CompilerParams(vmem_limit_bytes=room << 20),
        cost_estimate=pl.CostEstimate(flops=flops, bytes_accessed=1 << 20, transcendentals=0),
    )


def mm(a, b):
    return jnp.dot(a, b, preferred_element_type=F32)


def mm_t(a, b):
    return lax.dot_general(a, b, (((1,), (1,)), ((), ())), preferred_element_type=F32)


def normalize(values):
    values = values.astype(F32)
    average = jnp.mean(values, axis=-1, keepdims=True)
    centred = values - average
    spread = jnp.mean(centred * centred, axis=-1, keepdims=True)
    return (centred * lax.rsqrt(spread + EPSILON)).astype(BF16)


def wide(ref):
    return jnp.concatenate([ref[k] for k in range(ref.shape[0])], axis=-1)


def pack_kernel(rows, turned, order, *refs):
    sources, outs = refs[: rows + turned], refs[rows + turned :]
    tiles = []
    for ref in sources[:rows]:
        whole = ref[...]
        tiles.append([whole[:, k : k + 128] for k in range(0, whole.shape[1], 128)])
    for ref in sources[rows:]:
        whole = ref[...].astype(F32)
        tiles.append(
            [whole[k : k + 128, :].T.astype(BF16) for k in range(0, whole.shape[0], 128)]
        )
    for out, members in zip(outs, order):
        chunk = [tile for m in members for tile in tiles[m]]
        for t, tile in enumerate(chunk):
            for g in range(out.shape[0]):
                out[g, t] = tile


def regroup_kernel(counts, src, out):
    for z in range(4):
        first, column = 0, 0
        for count in counts:
            for h in range(4):
                for k in range(count):
                    out[z, :, column : column + 128] = src[z * 4 + h, first + k]
                    column += 128
            first += count


class Chunk:
    def __init__(self, widths):
        self.starts, self.widths, at = [], widths, 0
        for width in widths:
            self.starts.append(at)
            at += width

    def copies(self, k, dst, mine, theirs, core, sems):
        start, width = self.starts[k], self.widths[k]
        made = []
        for z in range(4):
            for n, (src, half) in enumerate(((mine, core), (theirs, 1 - core))):
                made.append(
                    pltpu.make_async_copy(
                        src.at[:, z, :, pl.ds(start, width)],
                        dst.at[z, :, half],
                        sems.at[z * 2 + n],
                    )
                )
        return made


CHUNK_A = Chunk((512, 512, 512))
CHUNK_B = Chunk((512, 512, 512, 512, 512))
CHUNK_C = Chunk((2048, 2048, 512, 512, 512, 512))


def weight_scratch(chunk, members):
    return [pltpu.VMEM((4, 16, 2, 8, chunk.widths[m]), BF16) for m in members] + [
        pltpu.SemaphoreType.DMA((len(members), 8))
    ]


class Weights:
    def __init__(self, chunk, members, pos, mine, theirs, buffers, sems):
        core = pos[1]
        self.buffers = buffers
        self.made = [
            chunk.copies(m, buffers[n], mine, theirs, core, sems.at[n])
            for n, m in enumerate(members)
        ]
        for group in self.made:
            for copy in group:
                copy.start()

    def get(self, n):
        for copy in self.made[n]:
            copy.wait()
        buffer = self.buffers[n]
        return buffer.reshape(D, buffer.shape[-1])[...]


def softmax_mix(queries, keys, values, dead):
    scores = jnp.where(dead, -1e30, mm_t(queries, keys))
    weights = jnp.exp(scores - jnp.max(scores, axis=-1, keepdims=True))
    weights = weights * (1.0 / jnp.sum(weights, axis=-1, keepdims=True))
    return mm(weights.astype(BF16), values)


def two_heads(queries, keys, values, dead):
    first = lax.broadcasted_iota(jnp.int32, queries.shape, 1) < HEAD_DIM
    zero = jnp.zeros_like(queries)
    low = softmax_mix(jnp.where(first, queries, zero), keys, values, dead)
    high = softmax_mix(jnp.where(first, zero, queries), keys, values, dead)
    return jnp.where(first, low, high).astype(BF16)


def inputs_kernel(pos, grid, mesh, mine, theirs, out, wk, wv, wq, sems):
    weights = Weights(CHUNK_A, (0, 1, 2), pos, mine, theirs, (wk, wv, wq), sems)
    grid_norm = normalize(wide(grid))
    mesh_norm = normalize(wide(mesh))
    rows = grid.shape[1]
    half = mesh.shape[1] // 2
    keys = mm(grid_norm, weights.get(0)).astype(BF16)
    for j in range(4):
        out[j, :rows, :PAIR] = keys[:, j * PAIR : (j + 1) * PAIR]
    values = mm(grid_norm, weights.get(1)).astype(BF16)
    for j in range(4):
        out[j, :rows, PAIR:] = values[:, j * PAIR : (j + 1) * PAIR]
    queries = (mm(mesh_norm, weights.get(2)) * SCALE).astype(BF16)
    for j in range(4):
        out[j, rows:, :PAIR] = queries[:half, j * PAIR : (j + 1) * PAIR]
        out[j, rows:, PAIR:] = queries[half:, j * PAIR : (j + 1) * PAIR]


def encode_kernel(pos, blocks, count, own, before, after, out, tiles, picked):
    rows = own.shape[1] - 32
    for j in range(2):
        for k in range(2):
            part = slice(k * TILE, (k + 1) * TILE)
            tiles[j * 2 + k] = before[j, part]
            tiles[12 + j * 2 + k] = after[j, part]
    for j in range(4):
        for k in range(rows // TILE):
            tiles[4 + j * 2 + k] = own[j, k * TILE : (k + 1) * TILE]
    start = pos[0] * 8 - 4
    slots = blocks.shape[1]
    column = lax.broadcasted_iota(jnp.int32, (TILE, slots * TILE), 1)
    for m in range(2):
        for s in range(slots):
            index = jnp.clip(blocks[m, s] - start, 0, 15)
            picked[s * TILE : (s + 1) * TILE, :] = tiles[index]
        queries = jnp.concatenate(
            [
                own[2 * m + g, rows:, side * PAIR : (side + 1) * PAIR]
                for g in range(2)
                for side in range(2)
            ],
            axis=0,
        )
        mixed = two_heads(queries, picked[:, :PAIR], picked[:, PAIR:], column >= count[m] * TILE)
        out[2 * m] = mixed[:64]
        out[2 * m + 1] = mixed[64:]


def first_kernel(pos, encoded, mesh, mine, theirs, qkv, kept, wo, wq, wk, wv, sems):
    weights = Weights(CHUNK_B, (0, 1, 2, 3), pos, mine, theirs, (wo, wq, wk, wv), sems)
    update = mm_t(wide(encoded), weights.get(0))
    mesh_one = (wide(mesh).astype(F32) + update).astype(BF16)
    kept[...] = mesh_one
    norm_one = normalize(mesh_one)
    for n, scaling in enumerate((SCALE, 1.0, 1.0)):
        part = (mm(norm_one, weights.get(1 + n)) * scaling).astype(BF16)
        for j in range(4):
            qkv[j, :, n * PAIR : (n + 1) * PAIR] = part[:, j * PAIR : (j + 1) * PAIR]


def window_kernel(pos, offsets, own, before, after, out, tiles, picked):
    for j in range(4):
        half = slice((j % 2) * 64, (j % 2) * 64 + 64)
        tiles[j // 2, half] = before[j]
        tiles[2 + j // 2, half] = own[j, :, PAIR:]
        tiles[4 + j // 2, half] = after[j]
    slots = offsets.shape[1]
    slot = lax.broadcasted_iota(jnp.int32, (TILE, slots * TILE), 1) // TILE
    for m in range(2):
        alive = jnp.zeros((TILE, slots * TILE), jnp.int32)
        for s in range(slots):
            offset = offsets[m, s]
            picked[s * TILE : (s + 1) * TILE, :] = tiles[jnp.clip(m + 2 + offset, 0, 5)]
            reached = pos[0] * 2 + m + offset
            live = jnp.where((reached >= 0) & (reached < pos[3]), 1, 0)
            alive = jnp.where(slot == s, live, alive)
        queries = jnp.concatenate([own[2 * m, :, :PAIR], own[2 * m + 1, :, :PAIR]], axis=0)
        mixed = two_heads(queries, picked[:, :PAIR], picked[:, PAIR:], alive == 0)
        out[2 * m] = mixed[:64]
        out[2 * m + 1] = mixed[64:]


def second_kernel(
    pos, windowed, kept, mine_b, theirs_b, mine_c, theirs_c, mesh_out, kv, wo, up, down, wk, wv,
    sems_b, sems_c
):
    near = Weights(CHUNK_B, (4,), pos, mine_b, theirs_b, (wo,), sems_b)
    far = Weights(CHUNK_C, (0, 1, 2, 3), pos, mine_c, theirs_c, (up, down, wk, wv), sems_c)
    update = mm_t(wide(windowed), near.get(0))
    mesh_two = (kept[...].astype(F32) + update).astype(BF16)
    hidden = mm(normalize(mesh_two), far.get(0))
    hidden = (0.5 * hidden * (1.0 + lax.erf(hidden * (2.0**-0.5)))).astype(BF16)
    result = (mesh_two.astype(F32) + mm_t(hidden, far.get(1))).astype(BF16)
    for j in range(4):
        mesh_out[j] = result[:, j * 256 : (j + 1) * 256]
    norm_three = normalize(result)
    keys = mm(norm_three, far.get(2)).astype(BF16)
    values = mm(norm_three, far.get(3)).astype(BF16)
    for g in range(4):
        kv[g, :, :512] = keys
        kv[g, :, 512:] = values


def decode_kernel(pos, blocks, count, grid, own, before, after, mine, theirs, out, wq, wo, tiles,
                  picked, sems):
    weights = Weights(CHUNK_C, (4, 5), pos, mine, theirs, (wq, wo), sems)
    tiles[0] = before[...]
    for j in range(4):
        half = slice((j % 2) * 64, (j % 2) * 64 + 64)
        tiles[1 + j // 2, half] = own[j]
    tiles[3] = after[...]
    grid_rows = wide(grid)
    queries = (mm(normalize(grid_rows), weights.get(0)) * SCALE).astype(BF16)
    start = pos[0] * 2 - 1
    slots = blocks.shape[1]
    column = lax.broadcasted_iota(jnp.int32, (TILE, slots * TILE), 1)
    mixtures = []
    for t in range(2):
        row = pos[2] * 2 + t
        for s in range(slots):
            index = jnp.clip(blocks[row, s] - start, 0, 3)
            picked[s * TILE : (s + 1) * TILE, :] = tiles[index]
        dead = column >= count[row] * TILE
        mixtures.append(
            jnp.concatenate(
                [
                    two_heads(
                        queries[t * TILE : (t + 1) * TILE, j * PAIR : (j + 1) * PAIR],
                        picked[:, j * PAIR : (j + 1) * PAIR],
                        picked[:, 512 + j * PAIR : 512 + (j + 1) * PAIR],
                        dead,
                    )
                    for j in range(4)
                ],
                axis=1,
            )
        )
    decoded = jnp.concatenate(mixtures, axis=0)
    result = (grid_rows.astype(F32) + mm_t(decoded, weights.get(1))).astype(BF16)
    for j in range(4):
        out[j] = result[:, j * 256 : (j + 1) * 256]


def exchange(x):
    return lax.all_to_all(x, "heads", 0, 0, tiled=True)


def halo(last, first):
    size = lax.axis_size(NODES)
    up = [(i, i + 1) for i in range(size - 1)]
    down = [(j, i) for i, j in up]
    return lax.ppermute(last, NODES, up), lax.ppermute(first, NODES, down)


def after_it(x, other):
    return lax.optimization_barrier((x, other))[0]


def over_cores(x):
    return lax.ppermute(x, "core", [(0, 1), (1, 0)])


def over_z(tiles, counts, name):
    arrived = lax.all_to_all(tiles, ("zh", "heads"), 0, 0, tiled=True)
    width = 4 * sum(counts) * 128
    (rows,) = call(
        functools.partial(regroup_kernel, counts), name, [(4, 8, width)], [in_vmem()]
    )(arrived)
    return rows


def local(
    grid_state,
    mesh_state,
    encoder_query,
    encoder_key,
    encoder_value,
    encoder_output,
    window_query,
    window_key,
    window_value,
    window_output,
    expand_weight,
    shrink_weight,
    decoder_query,
    decoder_key,
    decoder_value,
    decoder_output,
    encoder_blocks,
    encoder_count,
    window_offsets,
    decoder_blocks,
    decoder_count,
):
    position = lax.axis_index(NODES)
    mesh_tiles = lax.axis_size(NODES) * 2
    pos = jnp.stack(
        [position, lax.axis_index("core"), lax.axis_index("heads"), jnp.int32(mesh_tiles)]
    ).astype(jnp.int32)

    by_rows = [
        encoder_key, encoder_value, encoder_query, window_query, window_key, window_value,
        expand_weight, decoder_key, decoder_value, decoder_query,
    ]
    by_columns = [encoder_output, window_output, shrink_weight, decoder_output]
    order = ((0, 1, 2), (10, 3, 4, 5, 11), (6, 12, 7, 8, 9, 13))
    counts = ((1, 1, 1), (1, 1, 1, 1, 1), (4, 4, 1, 1, 1, 1))
    tiles_a, tiles_b, tiles_c = call(
        functools.partial(pack_kernel, len(by_rows), len(by_columns), order),
        "pack",
        [(16, sum(c), 8, 128) for c in counts],
        [in_vmem()] * 14,
    )(*by_rows, *by_columns)

    mesh = exchange(mesh_state.reshape(4, 64, 256))
    rows_a = over_z(tiles_a, counts[0], "regroup_a")
    mine_a = lax.all_to_all(
        jnp.broadcast_to(rows_a[None], (16, *rows_a.shape)), ("y", "x"), 0, 0, tiled=True
    )
    theirs_a = over_cores(mine_a)
    grid = exchange(after_it(grid_state, rows_a).reshape(4, 256, 256))
    rows_b = over_z(after_it(tiles_b, rows_a), counts[1], "regroup_b")
    mine_b = lax.all_gather(rows_b, ("y", "x"))
    rows_c = over_z(after_it(tiles_c, rows_b), counts[2], "regroup_c")
    mine_c = lax.all_gather(rows_c, ("y", "x"))

    (sent,) = call(
        inputs_kernel,
        "inputs",
        [(4, 288, 256)],
        [in_smem(), in_vmem(), in_vmem(), in_any(), in_any()],
        weight_scratch(CHUNK_A, (0, 1, 2)),
        room=16,
    )(pos, grid, mesh, mine_a, theirs_a)
    own = exchange(sent)
    before, after = halo(own[2:, :256], own[:2, :256])
    mine_b = after_it(mine_b, before)
    theirs_b = over_cores(mine_b)
    (sent,) = call(
        encode_kernel,
        "encode",
        [(4, 64, 128)],
        [in_smem()] * 3 + [in_vmem()] * 3,
        [pltpu.VMEM((16, TILE, 256), BF16), pltpu.VMEM((8 * TILE, 256), BF16)],
    )(pos, encoder_blocks, encoder_count, own, before, after)
    encoded = exchange(sent)
    sent, kept = call(
        first_kernel,
        "first",
        [(4, 64, 384), (64, D)],
        [in_smem(), in_vmem(), in_vmem(), in_any(), in_any()],
        weight_scratch(CHUNK_B, (0, 1, 2, 3)),
        room=16,
    )(pos, encoded, mesh, mine_b, theirs_b)
    own = exchange(sent)
    side = own[:, :, PAIR:]
    before, after = halo(side, side)
    mine_c = after_it(mine_c, before)
    theirs_c = over_cores(mine_c)
    (sent,) = call(
        window_kernel,
        "window",
        [(4, 64, 128)],
        [in_smem()] * 2 + [in_vmem()] * 3,
        [pltpu.VMEM((6, TILE, 256), BF16), pltpu.VMEM((4 * TILE, 256), BF16)],
    )(pos, window_offsets, own, before, after)
    windowed = exchange(sent)
    near, far = weight_scratch(CHUNK_B, (4,)), weight_scratch(CHUNK_C, (0, 1, 2, 3))
    sent, spread = call(
        second_kernel,
        "second",
        [(4, 64, 256), (4, 64, D)],
        [in_smem(), in_vmem(), in_vmem()] + [in_any()] * 4,
        near[:-1] + far[:-1] + [near[-1], far[-1]],
        room=24,
    )(pos, windowed, kept, mine_b, theirs_b, mine_c, theirs_c)
    own = exchange(spread)
    mesh_out = exchange(sent).reshape(256, 256)
    before, after = halo(own[2:].reshape(TILE, D), own[:2].reshape(TILE, D))
    pair = weight_scratch(CHUNK_C, (4, 5))
    (sent,) = call(
        decode_kernel,
        "decode",
        [(4, 256, 256)],
        [in_smem()] * 3 + [in_vmem()] * 4 + [in_any()] * 2,
        pair[:-1]
        + [pltpu.VMEM((4, TILE, D), BF16), pltpu.VMEM((3 * TILE, D), BF16), pair[-1]],
        room=20,
    )(pos, decoder_blocks, decoder_count, grid, own, before, after, mine_c, theirs_c)
    grid_out = exchange(sent).reshape(1024, 256)
    return grid_out, mesh_out


def solution(mesh):
    sizes = (4, 4, 4, 2)
    fine = Mesh(mesh.devices.reshape(*sizes, mesh.devices.shape[1]), (*NODES, "heads"))
    both, flipped = P(NODES, "heads"), P("heads", NODES)
    in_specs = (
        both, both, both, both, both, flipped, both, both, both, flipped, both, flipped,
        both, both, both, flipped,
        P(NODES, None), P(NODES), P(NODES, None), P(NODES, None), P(NODES),
    )
    return jax.shard_map(
        local, mesh=fine, in_specs=in_specs, out_specs=(both, both), check_vma=False
    )
```

```python
import functools

import jax
import jax.numpy as jnp
from jax import lax
from jax.experimental import pallas as pl
from jax.experimental.pallas import tpu as pltpu
from jax.sharding import Mesh
from jax.sharding import PartitionSpec as P


HEAD_DIM = 64
TILE = 128
PAIR = 2 * HEAD_DIM
D = 1024
SCALE = HEAD_DIM ** (-0.5)
EPSILON = 1e-05
NODES = ("zh", "y", "x", "core")
F32 = jnp.float32
BF16 = jnp.bfloat16


def in_vmem():
    return pl.BlockSpec(memory_space=pltpu.VMEM)


def in_smem():
    return pl.BlockSpec(memory_space=pltpu.SMEM)


def in_any():
    return pl.BlockSpec(memory_space=pltpu.HBM)


def call(kernel, outs, specs, scratch=(), flops=1 << 28, room=12):
    return pl.pallas_call(
        kernel,
        out_shape=tuple(jax.ShapeDtypeStruct(shape, BF16) for shape in outs),
        in_specs=list(specs),
        out_specs=tuple(in_vmem() for _ in outs),
        scratch_shapes=list(scratch),
        compiler_params=pltpu.CompilerParams(vmem_limit_bytes=room << 20),
        cost_estimate=pl.CostEstimate(flops=flops, bytes_accessed=1 << 20, transcendentals=0),
    )


def mm(a, b):
    return jnp.dot(a, b, preferred_element_type=F32)


def mm_t(a, b):
    return lax.dot_general(a, b, (((1,), (1,)), ((), ())), preferred_element_type=F32)


def normalize(values):
    values = values.astype(F32)
    average = jnp.mean(values, axis=-1, keepdims=True)
    centred = values - average
    spread = jnp.mean(centred * centred, axis=-1, keepdims=True)
    return (centred * lax.rsqrt(spread + EPSILON)).astype(BF16)


def wide(ref):
    return jnp.concatenate([ref[k] for k in range(ref.shape[0])], axis=-1)


def pack_kernel(*refs):
    *sources, out = refs
    t = 0
    for source in sources:
        whole = source[...]
        for k in range(0, whole.shape[1], 128):
            for g in range(out.shape[0]):
                out[g, t] = whole[:, k : k + 128]
            t += 1


def regroup_kernel(counts, src, *outs):
    first = 0
    for out, members in zip(outs, counts):
        column = 0
        for count in members:
            for h in range(4):
                for k in range(count):
                    for z in range(4):
                        out[z, :, column : column + 128] = src[z * 4 + h, first + k]
                    column += 128
            first += count


class Chunk:
    def __init__(self, widths):
        self.starts, self.widths, at = [], widths, 0
        for width in widths:
            self.starts.append(at)
            at += width

    def copies(self, k, dst, mine, theirs, core, sems):
        start, width = self.starts[k], self.widths[k]
        made = []
        for z in range(4):
            for n, (src, half) in enumerate(((mine, core), (theirs, 1 - core))):
                made.append(
                    pltpu.make_async_copy(
                        src.at[:, z, :, pl.ds(start, width)],
                        dst.at[z, :, half],
                        sems.at[z * 2 + n],
                    )
                )
        return made


CHUNK_A = Chunk((512, 512, 512))
CHUNK_B = Chunk((512, 512, 512, 512, 512))
CHUNK_C = Chunk((2048, 2048, 512, 512, 512, 512))


def weight_scratch(chunk, members):
    return [pltpu.VMEM((4, 16, 2, 8, chunk.widths[m]), BF16) for m in members] + [
        pltpu.SemaphoreType.DMA((len(members), 8))
    ]


class Weights:
    def __init__(self, chunk, members, pos, mine, theirs, buffers, sems):
        core = pos[1]
        self.buffers = buffers
        self.made = [
            chunk.copies(m, buffers[n], mine, theirs, core, sems.at[n])
            for n, m in enumerate(members)
        ]
        for group in self.made:
            for copy in group:
                copy.start()

    def get(self, n):
        for copy in self.made[n]:
            copy.wait()
        buffer = self.buffers[n]
        return buffer.reshape(D, buffer.shape[-1])[...]


def softmax_mix(queries, keys, values, dead):
    scores = jnp.where(dead, -1e30, mm_t(queries, keys))
    weights = jnp.exp(scores - jnp.max(scores, axis=-1, keepdims=True))
    weights = weights * (1.0 / jnp.sum(weights, axis=-1, keepdims=True))
    return mm(weights.astype(BF16), values)


def two_heads(queries, keys, values, dead):
    first = lax.broadcasted_iota(jnp.int32, queries.shape, 1) < HEAD_DIM
    zero = jnp.zeros_like(queries)
    low = softmax_mix(jnp.where(first, queries, zero), keys, values, dead)
    high = softmax_mix(jnp.where(first, zero, queries), keys, values, dead)
    return jnp.where(first, low, high).astype(BF16)


def inputs_kernel(
    pos, x0, x1, x2, x3, mine, theirs, out0, out1, out2, out3, grid, mesh, staged, wk, wv, wq, sems
):
    weights = Weights(CHUNK_A, (0, 1, 2), pos, mine, theirs, (wk, wv, wq), sems)
    head = pos[2]
    rows, half = grid.shape[1], mesh.shape[1] // 2
    for k, part in enumerate((x0, x1, x2, x3)):
        grid[head ^ k] = part[:rows, :]
        mesh[head ^ k] = part[rows:, :]
    grid_norm = normalize(wide(grid))
    mesh_norm = normalize(wide(mesh))
    keys = mm(grid_norm, weights.get(0)).astype(BF16)
    for j in range(4):
        staged[j, :rows, :PAIR] = keys[:, j * PAIR : (j + 1) * PAIR]
    values = mm(grid_norm, weights.get(1)).astype(BF16)
    for j in range(4):
        staged[j, :rows, PAIR:] = values[:, j * PAIR : (j + 1) * PAIR]
    queries = (mm(mesh_norm, weights.get(2)) * SCALE).astype(BF16)
    for j in range(4):
        staged[j, rows:, :PAIR] = queries[:half, j * PAIR : (j + 1) * PAIR]
        staged[j, rows:, PAIR:] = queries[half:, j * PAIR : (j + 1) * PAIR]
    for k, out in enumerate((out0, out1, out2, out3)):
        out[...] = staged[head ^ k]


def arrange_kernel(pos, x0, x1, x2, x3, own, last, first):
    head = pos[2]
    for k, part in enumerate((x0, x1, x2, x3)):
        own[head ^ k] = part[...]
    last[...] = own[2:, :256, :]
    first[...] = own[:2, :256, :]


def encode_kernel(pos, blocks, count, own, before, after, out, tiles, picked):
    rows = own.shape[1] - 32
    for j in range(2):
        for k in range(2):
            part = slice(k * TILE, (k + 1) * TILE)
            tiles[j * 2 + k] = before[j, part]
            tiles[12 + j * 2 + k] = after[j, part]
    for j in range(4):
        for k in range(rows // TILE):
            tiles[4 + j * 2 + k] = own[j, k * TILE : (k + 1) * TILE]
    start = pos[0] * 8 - 4
    slots = blocks.shape[1]
    column = lax.broadcasted_iota(jnp.int32, (TILE, slots * TILE), 1)
    for m in range(2):
        for s in range(slots):
            index = jnp.clip(blocks[m, s] - start, 0, 15)
            picked[s * TILE : (s + 1) * TILE, :] = tiles[index]
        queries = jnp.concatenate(
            [
                own[2 * m + g, rows:, side * PAIR : (side + 1) * PAIR]
                for g in range(2)
                for side in range(2)
            ],
            axis=0,
        )
        mixed = two_heads(queries, picked[:, :PAIR], picked[:, PAIR:], column >= count[m] * TILE)
        out[2 * m] = mixed[:64]
        out[2 * m + 1] = mixed[64:]


def first_kernel(pos, encoded, mesh, mine, theirs, qkv, kept, wo, wq, wk, wv, sems):
    weights = Weights(CHUNK_B, (0, 1, 2, 3), pos, mine, theirs, (wo, wq, wk, wv), sems)
    update = mm_t(wide(encoded), weights.get(0))
    mesh_one = (wide(mesh).astype(F32) + update).astype(BF16)
    kept[...] = mesh_one
    norm_one = normalize(mesh_one)
    for n, scaling in enumerate((SCALE, 1.0, 1.0)):
        part = (mm(norm_one, weights.get(1 + n)) * scaling).astype(BF16)
        for j in range(4):
            qkv[j, :, n * PAIR : (n + 1) * PAIR] = part[:, j * PAIR : (j + 1) * PAIR]


def window_kernel(pos, offsets, own, before, after, out, tiles, picked):
    for j in range(4):
        half = slice((j % 2) * 64, (j % 2) * 64 + 64)
        tiles[j // 2, half] = before[j]
        tiles[2 + j // 2, half] = own[j, :, PAIR:]
        tiles[4 + j // 2, half] = after[j]
    slots = offsets.shape[1]
    slot = lax.broadcasted_iota(jnp.int32, (TILE, slots * TILE), 1) // TILE
    for m in range(2):
        alive = jnp.zeros((TILE, slots * TILE), jnp.int32)
        for s in range(slots):
            offset = offsets[m, s]
            picked[s * TILE : (s + 1) * TILE, :] = tiles[jnp.clip(m + 2 + offset, 0, 5)]
            reached = pos[0] * 2 + m + offset
            live = jnp.where((reached >= 0) & (reached < pos[3]), 1, 0)
            alive = jnp.where(slot == s, live, alive)
        queries = jnp.concatenate([own[2 * m, :, :PAIR], own[2 * m + 1, :, :PAIR]], axis=0)
        mixed = two_heads(queries, picked[:, :PAIR], picked[:, PAIR:], alive == 0)
        out[2 * m] = mixed[:64]
        out[2 * m + 1] = mixed[64:]


def second_kernel(
    pos, windowed, kept, mine_b, theirs_b, mine_c, theirs_c, mesh_out, kv, wo, up, down, wk, wv,
    sems_b, sems_c
):
    near = Weights(CHUNK_B, (4,), pos, mine_b, theirs_b, (wo,), sems_b)
    far = Weights(CHUNK_C, (0, 1, 2, 3), pos, mine_c, theirs_c, (up, down, wk, wv), sems_c)
    update = mm_t(wide(windowed), near.get(0))
    mesh_two = (kept[...].astype(F32) + update).astype(BF16)
    hidden = mm(normalize(mesh_two), far.get(0))
    hidden = (0.5 * hidden * (1.0 + lax.erf(hidden * (2.0**-0.5)))).astype(BF16)
    result = (mesh_two.astype(F32) + mm_t(hidden, far.get(1))).astype(BF16)
    for j in range(4):
        mesh_out[j] = result[:, j * 256 : (j + 1) * 256]
    norm_three = normalize(result)
    keys = mm(norm_three, far.get(2)).astype(BF16)
    values = mm(norm_three, far.get(3)).astype(BF16)
    for g in range(4):
        kv[g, :, :512] = keys
        kv[g, :, 512:] = values


def decode_kernel(pos, blocks, count, grid, own, before, after, mine, theirs, out, wq, wo, tiles,
                  picked, sems):
    weights = Weights(CHUNK_C, (4, 5), pos, mine, theirs, (wq, wo), sems)
    tiles[0] = before[...]
    for j in range(4):
        half = slice((j % 2) * 64, (j % 2) * 64 + 64)
        tiles[1 + j // 2, half] = own[j]
    tiles[3] = after[...]
    grid_rows = wide(grid)
    queries = (mm(normalize(grid_rows), weights.get(0)) * SCALE).astype(BF16)
    start = pos[0] * 2 - 1
    slots = blocks.shape[1]
    column = lax.broadcasted_iota(jnp.int32, (TILE, slots * TILE), 1)
    mixtures = []
    for t in range(2):
        row = pos[2] * 2 + t
        for s in range(slots):
            index = jnp.clip(blocks[row, s] - start, 0, 3)
            picked[s * TILE : (s + 1) * TILE, :] = tiles[index]
        dead = column >= count[row] * TILE
        mixtures.append(
            jnp.concatenate(
                [
                    two_heads(
                        queries[t * TILE : (t + 1) * TILE, j * PAIR : (j + 1) * PAIR],
                        picked[:, j * PAIR : (j + 1) * PAIR],
                        picked[:, 512 + j * PAIR : 512 + (j + 1) * PAIR],
                        dead,
                    )
                    for j in range(4)
                ],
                axis=1,
            )
        )
    decoded = jnp.concatenate(mixtures, axis=0)
    result = (grid_rows.astype(F32) + mm_t(decoded, weights.get(1))).astype(BF16)
    for j in range(4):
        out[j] = result[:, j * 256 : (j + 1) * 256]


def exchange(x):
    return lax.all_to_all(x, "heads", 0, 0, tiled=True)


def halo(last, first):
    size = lax.axis_size(NODES)
    up = [(i, i + 1) for i in range(size - 1)]
    down = [(j, i) for i, j in up]
    return lax.ppermute(last, NODES, up), lax.ppermute(first, NODES, down)


def after_it(x, other):
    return lax.optimization_barrier((x, other))[0]


def in_hbm(x):
    return pltpu.with_memory_space_constraint(x, pltpu.HBM)


def over_cores(x):
    return lax.ppermute(x, "core", [(0, 1), (1, 0)])


def trade(parts):
    out = [parts[0]]
    for k in range(1, 4):
        out.append(lax.ppermute(parts[k], "heads", [(i, i ^ k) for i in range(4)]))
    return out


def pack(sources):
    width = sum(w.shape[1] // 128 for w in sources)
    (tiles,) = call(
        pack_kernel, [(16, width, 8, 128)], [in_vmem()] * len(sources), room=56
    )(*sources)
    return tiles


def to_everyone(x):
    return jnp.broadcast_to(x[None], (16, *x.shape))


def over_plane(x):
    return lax.all_to_all(x, ("y", "x"), 0, 0, tiled=True)


def over_z(tiles, counts):
    arrived = lax.all_to_all(tiles, ("zh", "heads"), 0, 0, tiled=True)
    return call(
        functools.partial(regroup_kernel, counts),
        [(4, 8, 4 * sum(count) * 128) for count in counts],
        [in_vmem()],
    )(arrived)


def local(
    grid_state,
    mesh_state,
    encoder_query,
    encoder_key,
    encoder_value,
    encoder_output,
    window_query,
    window_key,
    window_value,
    window_output,
    expand_weight,
    shrink_weight,
    decoder_query,
    decoder_key,
    decoder_value,
    decoder_output,
    encoder_blocks,
    encoder_count,
    window_offsets,
    decoder_blocks,
    decoder_count,
):
    position = lax.axis_index(NODES)
    mesh_tiles = lax.axis_size(NODES) * 2
    pos = jnp.stack(
        [position, lax.axis_index("core"), lax.axis_index("heads"), jnp.int32(mesh_tiles)]
    ).astype(jnp.int32)

    counts = ((1, 1, 1), (1, 1, 1, 1, 1), (4, 4, 1, 1, 1, 1))
    tiles = pack(
        (
            encoder_key, encoder_value, encoder_query, encoder_output.T, window_query, window_key,
            window_value, window_output.T, expand_weight, shrink_weight.T, decoder_key,
            decoder_value, decoder_query, decoder_output.T,
        )
    )
    rows_a, rows_b, rows_c = over_z(tiles, counts)
    copies_a = to_everyone(rows_a)
    mine_a = over_plane(copies_a)
    theirs_a = over_cores(mine_a)
    mine_c = lax.all_gather(rows_c, ("y", "x"))

    head = lax.axis_index("heads")
    both = [
        jnp.concatenate(
            [
                lax.dynamic_index_in_dim(after_it(x, copies_a).reshape(4, -1, 256), head ^ k, 0, False)
                for x in (grid_state, mesh_state)
            ]
        )
        for k in range(4)
    ]
    *sent, grid, mesh = call(
        inputs_kernel,
        [(288, 256)] * 4 + [(4, 256, 256), (4, 64, 256)],
        [in_smem()] + [in_vmem()] * 4 + [in_any(), in_any()],
        [pltpu.VMEM((4, 288, 256), BF16)] + weight_scratch(CHUNK_A, (0, 1, 2)),
        room=16,
    )(pos, *trade(both), mine_a, theirs_a)
    copies_b = to_everyone(after_it(rows_b, mine_a))
    mine_b = over_plane(copies_b)
    own, last, first = call(
        arrange_kernel,
        [(4, 288, 256), (2, 256, 256), (2, 256, 256)],
        [in_smem()] + [in_vmem()] * 4,
        room=8,
    )(pos, *trade(sent))
    before, after = halo(last, first)
    theirs_b = over_cores(mine_b)
    mine_b, theirs_b = in_hbm(mine_b), in_hbm(theirs_b)
    (sent,) = call(
        encode_kernel,
        [(4, 64, 128)],
        [in_smem()] * 3 + [in_vmem()] * 3,
        [pltpu.VMEM((16, TILE, 256), BF16), pltpu.VMEM((8 * TILE, 256), BF16)],
    )(pos, encoder_blocks, encoder_count, own, before, after)
    encoded = exchange(sent)
    sent, kept = call(
        first_kernel,
        [(4, 64, 384), (64, D)],
        [in_smem(), in_vmem(), in_vmem(), in_any(), in_any()],
        weight_scratch(CHUNK_B, (0, 1, 2, 3)),
        room=16,
    )(pos, encoded, mesh, mine_b, theirs_b)
    own = exchange(sent)
    side = own[:, :, PAIR:]
    before, after = halo(side, side)
    mine_c = after_it(mine_c, (before, after))
    theirs_c = over_cores(mine_c)
    mine_c, theirs_c = in_hbm(mine_c), in_hbm(theirs_c)
    (sent,) = call(
        window_kernel,
        [(4, 64, 128)],
        [in_smem()] * 2 + [in_vmem()] * 3,
        [pltpu.VMEM((6, TILE, 256), BF16), pltpu.VMEM((4 * TILE, 256), BF16)],
    )(pos, window_offsets, own, before, after)
    windowed = exchange(sent)
    near, far = weight_scratch(CHUNK_B, (4,)), weight_scratch(CHUNK_C, (0, 1, 2, 3))
    sent, spread = call(
        second_kernel,
        [(4, 64, 256), (4, 64, D)],
        [in_smem(), in_vmem(), in_vmem()] + [in_any()] * 4,
        near[:-1] + far[:-1] + [near[-1], far[-1]],
        room=24,
    )(pos, windowed, kept, mine_b, theirs_b, mine_c, theirs_c)
    own = exchange(spread)
    mesh_out = exchange(sent).reshape(256, 256)
    before, after = halo(own[2:].reshape(TILE, D), own[:2].reshape(TILE, D))
    pair = weight_scratch(CHUNK_C, (4, 5))
    (sent,) = call(
        decode_kernel,
        [(4, 256, 256)],
        [in_smem()] * 3 + [in_vmem()] * 4 + [in_any()] * 2,
        pair[:-1]
        + [pltpu.VMEM((4, TILE, D), BF16), pltpu.VMEM((3 * TILE, D), BF16), pair[-1]],
        room=20,
    )(pos, decoder_blocks, decoder_count, grid, own, before, after, mine_c, theirs_c)
    grid_out = exchange(sent).reshape(1024, 256)
    return grid_out, mesh_out


def solution(mesh):
    sizes = (4, 4, 4, 2)
    fine = Mesh(mesh.devices.reshape(*sizes, mesh.devices.shape[1]), (*NODES, "heads"))
    both, flipped = P(NODES, "heads"), P("heads", NODES)
    in_specs = (
        both, both, both, both, both, flipped, both, both, both, flipped, both, flipped,
        both, both, both, flipped,
        P(NODES, None), P(NODES), P(NODES, None), P(NODES, None), P(NODES),
    )
    return jax.shard_map(
        local, mesh=fine, in_specs=in_specs, out_specs=(both, both), check_vma=False
    )
```

```python
import functools

import jax
import jax.numpy as jnp
from jax import lax
from jax.experimental import pallas as pl
from jax.experimental.pallas import tpu as pltpu
from jax.sharding import Mesh
from jax.sharding import PartitionSpec as P


HEAD_DIM = 64
TILE = 128
PAIR = 2 * HEAD_DIM
D = 1024
SCALE = HEAD_DIM ** (-0.5)
EPSILON = 1e-05
NODES = ("zh", "y", "x", "core")
F32 = jnp.float32
BF16 = jnp.bfloat16


def in_vmem():
    return pl.BlockSpec(memory_space=pltpu.VMEM)


def in_smem():
    return pl.BlockSpec(memory_space=pltpu.SMEM)


def in_any():
    return pl.BlockSpec(memory_space=pltpu.HBM)


def call(kernel, outs, specs, scratch=(), flops=1 << 28, room=12):
    return pl.pallas_call(
        kernel,
        out_shape=tuple(jax.ShapeDtypeStruct(shape, BF16) for shape in outs),
        in_specs=list(specs),
        out_specs=tuple(in_vmem() for _ in outs),
        scratch_shapes=list(scratch),
        compiler_params=pltpu.CompilerParams(vmem_limit_bytes=room << 20),
        cost_estimate=pl.CostEstimate(flops=flops, bytes_accessed=1 << 20, transcendentals=0),
    )


def mm(a, b):
    return jnp.dot(a, b, preferred_element_type=F32)


def mm_t(a, b):
    return lax.dot_general(a, b, (((1,), (1,)), ((), ())), preferred_element_type=F32)


def normalize(values):
    values = values.astype(F32)
    average = jnp.mean(values, axis=-1, keepdims=True)
    centred = values - average
    spread = jnp.mean(centred * centred, axis=-1, keepdims=True)
    return (centred * lax.rsqrt(spread + EPSILON)).astype(BF16)


def wide(ref):
    return jnp.concatenate([ref[k] for k in range(ref.shape[0])], axis=-1)


def pack_kernel(*refs):
    *sources, near, far = refs
    t = 0
    for source in sources:
        whole = source[...]
        for k in range(0, whole.shape[1], 128):
            tile = whole[:, k : k + 128]
            if t < near.shape[1]:
                for g in range(near.shape[0]):
                    near[g, t] = tile
            else:
                far[t - near.shape[1]] = tile
            t += 1


def regroup_near_kernel(src, out):
    for t in range(src.shape[2]):
        for h in range(4):
            for z in range(4):
                tile = src[h, z, t]
                column = (4 * t + h) * 128
                for g in range(out.shape[0]):
                    out[g, z, :, column : column + 128] = tile


def stack_kernel(pos, x0, x1, x2, x3, out):
    for k, part in enumerate((x0, x1, x2, x3)):
        out[(pos[4] + 4 - k) % 4] = part[...]


def regroup_far_kernel(counts, pos, x0, x1, x2, x3, *outs):
    for n, part in enumerate((x0, x1, x2, x3)):
        h = pos[2] ^ n
        first = 0
        for out, members in zip(outs, counts):
            column = 0
            for count in members:
                for k in range(count):
                    at = pl.multiple_of((column + h * count + k) * 128, 128)
                    for z in range(4):
                        out[z, :, pl.ds(at, 128)] = part[z, first + k]
                first += count
                column += 4 * count


class Chunk:
    def __init__(self, widths):
        self.starts, self.widths, at = [], widths, 0
        for width in widths:
            self.starts.append(at)
            at += width

    def copies(self, k, dst, mine, theirs, core, sems):
        start, width = self.starts[k], self.widths[k]
        made = []
        for z in range(4):
            for n, (src, half) in enumerate(((mine, core), (theirs, 1 - core))):
                made.append(
                    pltpu.make_async_copy(
                        src.at[:, z, :, pl.ds(start, width)],
                        dst.at[z, :, half],
                        sems.at[z * 2 + n],
                    )
                )
        return made


CHUNK_A = Chunk((512, 512, 512))
CHUNK_B = Chunk((512, 512, 512, 512, 512))
CHUNK_C = Chunk((2048, 2048, 512, 512, 512, 512))


def weight_scratch(chunk, members):
    return [pltpu.VMEM((4, 16, 2, 8, chunk.widths[m]), BF16) for m in members] + [
        pltpu.SemaphoreType.DMA((len(members), 8))
    ]


class Weights:
    def __init__(self, chunk, members, pos, mine, theirs, buffers, sems):
        core = pos[1]
        self.buffers = buffers
        self.made = [
            chunk.copies(m, buffers[n], mine, theirs, core, sems.at[n])
            for n, m in enumerate(members)
        ]
        for group in self.made:
            for copy in group:
                copy.start()

    def get(self, n):
        for copy in self.made[n]:
            copy.wait()
        buffer = self.buffers[n]
        return buffer.reshape(D, buffer.shape[-1])[...]


def softmax_mix(queries, keys, values, dead):
    scores = jnp.where(dead, -1e30, mm_t(queries, keys))
    weights = jnp.exp(scores - jnp.max(scores, axis=-1, keepdims=True))
    weights = weights * (1.0 / jnp.sum(weights, axis=-1, keepdims=True))
    return mm(weights.astype(BF16), values)


def two_heads(queries, keys, values, dead):
    first = lax.broadcasted_iota(jnp.int32, queries.shape, 1) < HEAD_DIM
    zero = jnp.zeros_like(queries)
    low = softmax_mix(jnp.where(first, queries, zero), keys, values, dead)
    high = softmax_mix(jnp.where(first, zero, queries), keys, values, dead)
    return jnp.where(first, low, high).astype(BF16)


def inputs_kernel(
    pos, x0, x1, x2, x3, mine, theirs, out0, out1, out2, out3, grid, mesh, staged, wk, wv, wq, sems
):
    weights = Weights(CHUNK_A, (0, 1, 2), pos, mine, theirs, (wk, wv, wq), sems)
    head = pos[2]
    rows, half = grid.shape[1], mesh.shape[1] // 2
    for k, part in enumerate((x0, x1, x2, x3)):
        grid[head ^ k] = part[:rows, :]
        mesh[head ^ k] = part[rows:, :]
    grid_norm = normalize(wide(grid))
    mesh_norm = normalize(wide(mesh))
    keys = mm(grid_norm, weights.get(0)).astype(BF16)
    for j in range(4):
        staged[j, :rows, :PAIR] = keys[:, j * PAIR : (j + 1) * PAIR]
    values = mm(grid_norm, weights.get(1)).astype(BF16)
    for j in range(4):
        staged[j, :rows, PAIR:] = values[:, j * PAIR : (j + 1) * PAIR]
    queries = (mm(mesh_norm, weights.get(2)) * SCALE).astype(BF16)
    for j in range(4):
        staged[j, rows:, :PAIR] = queries[:half, j * PAIR : (j + 1) * PAIR]
        staged[j, rows:, PAIR:] = queries[half:, j * PAIR : (j + 1) * PAIR]
    for k, out in enumerate((out0, out1, out2, out3)):
        out[...] = staged[head ^ k]


def arrange_kernel(pos, x0, x1, x2, x3, own, last, first):
    head = pos[2]
    for k, part in enumerate((x0, x1, x2, x3)):
        own[head ^ k] = part[...]
    last[...] = own[2:, :256, :]
    first[...] = own[:2, :256, :]


def encode_kernel(pos, blocks, count, own, before, after, out, tiles, picked):
    rows = own.shape[1] - 32
    for j in range(2):
        for k in range(2):
            part = slice(k * TILE, (k + 1) * TILE)
            tiles[j * 2 + k] = before[j, part]
            tiles[12 + j * 2 + k] = after[j, part]
    for j in range(4):
        for k in range(rows // TILE):
            tiles[4 + j * 2 + k] = own[j, k * TILE : (k + 1) * TILE]
    start = pos[0] * 8 - 4
    slots = blocks.shape[1]
    column = lax.broadcasted_iota(jnp.int32, (TILE, slots * TILE), 1)
    for m in range(2):
        for s in range(slots):
            index = jnp.clip(blocks[m, s] - start, 0, 15)
            picked[s * TILE : (s + 1) * TILE, :] = tiles[index]
        queries = jnp.concatenate(
            [
                own[2 * m + g, rows:, side * PAIR : (side + 1) * PAIR]
                for g in range(2)
                for side in range(2)
            ],
            axis=0,
        )
        mixed = two_heads(queries, picked[:, :PAIR], picked[:, PAIR:], column >= count[m] * TILE)
        out[2 * m] = mixed[:64]
        out[2 * m + 1] = mixed[64:]


def first_kernel(pos, encoded, mesh, mine, theirs, qkv, kept, wo, wq, wk, wv, sems):
    weights = Weights(CHUNK_B, (0, 1, 2, 3), pos, mine, theirs, (wo, wq, wk, wv), sems)
    update = mm_t(wide(encoded), weights.get(0))
    mesh_one = (wide(mesh).astype(F32) + update).astype(BF16)
    kept[...] = mesh_one
    norm_one = normalize(mesh_one)
    for n, scaling in enumerate((SCALE, 1.0, 1.0)):
        part = (mm(norm_one, weights.get(1 + n)) * scaling).astype(BF16)
        for j in range(4):
            qkv[j, :, n * PAIR : (n + 1) * PAIR] = part[:, j * PAIR : (j + 1) * PAIR]


def window_kernel(pos, offsets, own, before, after, out, tiles, picked):
    for j in range(4):
        half = slice((j % 2) * 64, (j % 2) * 64 + 64)
        tiles[j // 2, half] = before[j]
        tiles[2 + j // 2, half] = own[j, :, PAIR:]
        tiles[4 + j // 2, half] = after[j]
    slots = offsets.shape[1]
    slot = lax.broadcasted_iota(jnp.int32, (TILE, slots * TILE), 1) // TILE
    for m in range(2):
        alive = jnp.zeros((TILE, slots * TILE), jnp.int32)
        for s in range(slots):
            offset = offsets[m, s]
            picked[s * TILE : (s + 1) * TILE, :] = tiles[jnp.clip(m + 2 + offset, 0, 5)]
            reached = pos[0] * 2 + m + offset
            live = jnp.where((reached >= 0) & (reached < pos[3]), 1, 0)
            alive = jnp.where(slot == s, live, alive)
        queries = jnp.concatenate([own[2 * m, :, :PAIR], own[2 * m + 1, :, :PAIR]], axis=0)
        mixed = two_heads(queries, picked[:, :PAIR], picked[:, PAIR:], alive == 0)
        out[2 * m] = mixed[:64]
        out[2 * m + 1] = mixed[64:]


def second_kernel(
    pos, windowed, kept, mine_b, theirs_b, mine_c, theirs_c, mesh_out, kv, wo, up, down, wk, wv,
    sems_b, sems_c
):
    near = Weights(CHUNK_B, (4,), pos, mine_b, theirs_b, (wo,), sems_b)
    far = Weights(CHUNK_C, (0, 1, 2, 3), pos, mine_c, theirs_c, (up, down, wk, wv), sems_c)
    update = mm_t(wide(windowed), near.get(0))
    mesh_two = (kept[...].astype(F32) + update).astype(BF16)
    hidden = mm(normalize(mesh_two), far.get(0))
    hidden = (0.5 * hidden * (1.0 + lax.erf(hidden * (2.0**-0.5)))).astype(BF16)
    result = (mesh_two.astype(F32) + mm_t(hidden, far.get(1))).astype(BF16)
    for j in range(4):
        mesh_out[j] = result[:, j * 256 : (j + 1) * 256]
    norm_three = normalize(result)
    keys = mm(norm_three, far.get(2)).astype(BF16)
    values = mm(norm_three, far.get(3)).astype(BF16)
    for g in range(4):
        kv[g, :, :512] = keys
        kv[g, :, 512:] = values


def queries_kernel(pos, grid, mine, theirs, out, wq, sems):
    weights = Weights(CHUNK_C, (4,), pos, mine, theirs, (wq,), sems)
    out[...] = (mm(normalize(wide(grid)), weights.get(0)) * SCALE).astype(BF16)


def decode_kernel(pos, blocks, count, grid, queries, own, before, after, mine, theirs, out, wo,
                  tiles, picked, sems):
    weights = Weights(CHUNK_C, (5,), pos, mine, theirs, (wo,), sems)
    tiles[0] = before[...]
    for j in range(4):
        half = slice((j % 2) * 64, (j % 2) * 64 + 64)
        tiles[1 + j // 2, half] = own[j]
    tiles[3] = after[...]
    start = pos[0] * 2 - 1
    slots = blocks.shape[1]
    column = lax.broadcasted_iota(jnp.int32, (TILE, slots * TILE), 1)
    mixtures = []
    for t in range(2):
        row = pos[2] * 2 + t
        for s in range(slots):
            index = jnp.clip(blocks[row, s] - start, 0, 3)
            picked[s * TILE : (s + 1) * TILE, :] = tiles[index]
        dead = column >= count[row] * TILE
        mixtures.append(
            jnp.concatenate(
                [
                    two_heads(
                        queries[t * TILE : (t + 1) * TILE, j * PAIR : (j + 1) * PAIR],
                        picked[:, j * PAIR : (j + 1) * PAIR],
                        picked[:, 512 + j * PAIR : 512 + (j + 1) * PAIR],
                        dead,
                    )
                    for j in range(4)
                ],
                axis=1,
            )
        )
    decoded = jnp.concatenate(mixtures, axis=0)
    result = (wide(grid).astype(F32) + mm_t(decoded, weights.get(0))).astype(BF16)
    for j in range(4):
        out[j] = result[:, j * 256 : (j + 1) * 256]


def exchange(x):
    return lax.all_to_all(x, "heads", 0, 0, tiled=True)


def halo(last, first):
    size = lax.axis_size(NODES)
    up = [(i, i + 1) for i in range(size - 1)]
    down = [(j, i) for i, j in up]
    return lax.ppermute(last, NODES, up), lax.ppermute(first, NODES, down)


def after_it(x, other):
    return lax.optimization_barrier((x, other))[0]


def in_hbm(x):
    return pltpu.with_memory_space_constraint(x, pltpu.HBM)


def over_cores(x):
    return lax.ppermute(x, "core", [(0, 1), (1, 0)])


def trade(parts):
    out = [parts[0]]
    for k in range(1, 4):
        out.append(lax.ppermute(parts[k], "heads", [(i, i ^ k) for i in range(4)]))
    return out


def pack(sources):
    return call(
        pack_kernel, [(4, 3, 8, 128), (17, 8, 128)], [in_vmem()] * len(sources), room=56
    )(*sources)


def to_everyone(x):
    return jnp.broadcast_to(x[None], (16, *x.shape))


def over_plane(x):
    return lax.all_to_all(x, ("y", "x"), 0, 0, tiled=True)


def local(
    grid_state,
    mesh_state,
    encoder_query,
    encoder_key,
    encoder_value,
    encoder_output,
    window_query,
    window_key,
    window_value,
    window_output,
    expand_weight,
    shrink_weight,
    decoder_query,
    decoder_key,
    decoder_value,
    decoder_output,
    encoder_blocks,
    encoder_count,
    window_offsets,
    decoder_blocks,
    decoder_count,
):
    position = lax.axis_index(NODES)
    mesh_tiles = lax.axis_size(NODES) * 2
    pos = jnp.stack(
        [position, lax.axis_index("core"), lax.axis_index("heads"), jnp.int32(mesh_tiles),
         lax.axis_index("zh")]
    ).astype(jnp.int32)

    counts = ((1, 1, 1, 1, 1), (4, 4, 1, 1, 1, 1))
    near, far = pack(
        (
            encoder_key, encoder_value, encoder_query, encoder_output.T, window_query, window_key,
            window_value, window_output.T, expand_weight, shrink_weight.T, decoder_key,
            decoder_value, decoder_query, decoder_output.T,
        )
    )
    near = lax.all_to_all(near, "zh", 0, 0, tiled=True)
    near = exchange(jnp.broadcast_to(near[None], (4, *near.shape)))
    (copies_a,) = call(regroup_near_kernel, [(16, 4, 8, 1536)], [in_vmem()], room=8)(near)
    mine_a = over_plane(copies_a)
    theirs_a = over_cores(mine_a)
    mine_a, theirs_a = in_hbm(mine_a), in_hbm(theirs_a)

    far = [after_it(far, copies_a)] * 4
    far = [far[0]] + [
        lax.ppermute(far[k], "zh", [(i, (i + k) % 4) for i in range(4)]) for k in range(1, 4)
    ]
    (far,) = call(stack_kernel, [(4, 17, 8, 128)], [in_smem()] + [in_vmem()] * 4, room=4)(pos, *far)
    rows_b, rows_c = call(
        functools.partial(regroup_far_kernel, counts),
        [(4, 8, 2560), (4, 8, 6144)],
        [in_smem()] + [in_vmem()] * 4,
        room=8,
    )(pos, *trade([far] * 4))
    mine_c = lax.all_gather(rows_c, ("y", "x"))

    head = lax.axis_index("heads")
    both = [
        jnp.concatenate(
            [
                lax.dynamic_index_in_dim(after_it(x, copies_a).reshape(4, -1, 256), head ^ k, 0, False)
                for x in (grid_state, mesh_state)
            ]
        )
        for k in range(4)
    ]
    *sent, grid, mesh = call(
        inputs_kernel,
        [(288, 256)] * 4 + [(4, 256, 256), (4, 64, 256)],
        [in_smem()] + [in_vmem()] * 4 + [in_any(), in_any()],
        [pltpu.VMEM((4, 288, 256), BF16)] + weight_scratch(CHUNK_A, (0, 1, 2)),
        room=16,
    )(pos, *trade(both), mine_a, theirs_a)
    copies_b = to_everyone(after_it(rows_b, mine_a))
    mine_b = over_plane(copies_b)
    own, last, first = call(
        arrange_kernel,
        [(4, 288, 256), (2, 256, 256), (2, 256, 256)],
        [in_smem()] + [in_vmem()] * 4,
        room=8,
    )(pos, *trade(sent))
    before, after = halo(last, first)
    theirs_b = over_cores(mine_b)
    mine_b, theirs_b = in_hbm(mine_b), in_hbm(theirs_b)
    (sent,) = call(
        encode_kernel,
        [(4, 64, 128)],
        [in_smem()] * 3 + [in_vmem()] * 3,
        [pltpu.VMEM((16, TILE, 256), BF16), pltpu.VMEM((8 * TILE, 256), BF16)],
    )(pos, encoder_blocks, encoder_count, own, before, after)
    encoded = exchange(sent)
    sent, kept = call(
        first_kernel,
        [(4, 64, 384), (64, D)],
        [in_smem(), in_vmem(), in_vmem(), in_any(), in_any()],
        weight_scratch(CHUNK_B, (0, 1, 2, 3)),
        room=16,
    )(pos, encoded, mesh, mine_b, theirs_b)
    own = exchange(sent)
    side = own[:, :, PAIR:]
    before, after = halo(side, side)
    mine_c = after_it(mine_c, (before, after))
    theirs_c = over_cores(mine_c)
    mine_c, theirs_c = in_hbm(mine_c), in_hbm(theirs_c)
    (sent,) = call(
        window_kernel,
        [(4, 64, 128)],
        [in_smem()] * 2 + [in_vmem()] * 3,
        [pltpu.VMEM((6, TILE, 256), BF16), pltpu.VMEM((4 * TILE, 256), BF16)],
    )(pos, window_offsets, own, before, after)
    windowed = exchange(sent)
    near, far = weight_scratch(CHUNK_B, (4,)), weight_scratch(CHUNK_C, (0, 1, 2, 3))
    sent, spread = call(
        second_kernel,
        [(4, 64, 256), (4, 64, D)],
        [in_smem(), in_vmem(), in_vmem()] + [in_any()] * 4,
        near[:-1] + far[:-1] + [near[-1], far[-1]],
        room=24,
    )(pos, windowed, kept, mine_b, theirs_b, mine_c, theirs_c)
    own = exchange(spread)
    before, after = halo(own[2:].reshape(TILE, D), own[:2].reshape(TILE, D))
    mesh_out = exchange(sent).reshape(256, 256)
    (queries,) = call(
        queries_kernel,
        [(256, 512)],
        [in_smem(), in_vmem()] + [in_any()] * 2,
        weight_scratch(CHUNK_C, (4,)),
        room=12,
    )(pos, grid, mine_c, theirs_c)
    last = weight_scratch(CHUNK_C, (5,))
    (sent,) = call(
        decode_kernel,
        [(4, 256, 256)],
        [in_smem()] * 3 + [in_vmem()] * 5 + [in_any()] * 2,
        last[:-1]
        + [pltpu.VMEM((4, TILE, D), BF16), pltpu.VMEM((3 * TILE, D), BF16), last[-1]],
        room=16,
    )(pos, decoder_blocks, decoder_count, grid, queries, own, before, after, mine_c, theirs_c)
    grid_out = exchange(sent).reshape(1024, 256)
    return grid_out, mesh_out


def solution(mesh):
    sizes = (4, 4, 4, 2)
    fine = Mesh(mesh.devices.reshape(*sizes, mesh.devices.shape[1]), (*NODES, "heads"))
    both, flipped = P(NODES, "heads"), P("heads", NODES)
    in_specs = (
        both, both, both, both, both, flipped, both, both, both, flipped, both, flipped,
        both, both, both, flipped,
        P(NODES, None), P(NODES), P(NODES, None), P(NODES, None), P(NODES),
    )
    return jax.shard_map(
        local, mesh=fine, in_specs=in_specs, out_specs=(both, both), check_vma=False
    )
```

```python
import functools

import jax
import jax.numpy as jnp
from jax import lax
from jax.experimental import pallas as pl
from jax.experimental.pallas import tpu as pltpu
from jax.sharding import Mesh
from jax.sharding import PartitionSpec as P


HEAD_DIM = 64
TILE = 128
PAIR = 2 * HEAD_DIM
D = 1024
SCALE = HEAD_DIM ** (-0.5)
EPSILON = 1e-05
NODES = ("zh", "y", "x", "core")
F32 = jnp.float32
BF16 = jnp.bfloat16


def in_vmem():
    return pl.BlockSpec(memory_space=pltpu.VMEM)


def in_smem():
    return pl.BlockSpec(memory_space=pltpu.SMEM)


def in_any():
    return pl.BlockSpec(memory_space=pltpu.HBM)


def call(kernel, outs, specs, scratch=(), flops=1 << 28, room=12):
    return pl.pallas_call(
        kernel,
        out_shape=tuple(jax.ShapeDtypeStruct(shape, BF16) for shape in outs),
        in_specs=list(specs),
        out_specs=tuple(in_vmem() for _ in outs),
        scratch_shapes=list(scratch),
        compiler_params=pltpu.CompilerParams(vmem_limit_bytes=room << 20),
        cost_estimate=pl.CostEstimate(flops=flops, bytes_accessed=1 << 20, transcendentals=0),
    )


def mm(a, b):
    return jnp.dot(a, b, preferred_element_type=F32)


def mm_t(a, b):
    return lax.dot_general(a, b, (((1,), (1,)), ((), ())), preferred_element_type=F32)


def normalize(values):
    values = values.astype(F32)
    average = jnp.mean(values, axis=-1, keepdims=True)
    centred = values - average
    spread = jnp.mean(centred * centred, axis=-1, keepdims=True)
    return (centred * lax.rsqrt(spread + EPSILON)).astype(BF16)


def wide(ref):
    return jnp.concatenate([ref[k] for k in range(ref.shape[0])], axis=-1)


def pack_kernel(*refs):
    *sources, out = refs
    t = 0
    for source in sources:
        whole = source[...]
        for k in range(0, whole.shape[1], 128):
            for g in range(out.shape[0]):
                out[g, t] = whole[:, k : k + 128]
            t += 1


def regroup_kernel(counts, src, near, far):
    first = 0
    for out, members in zip((near, far), counts):
        column = 0
        for count in members:
            for h in range(4):
                for k in range(count):
                    for z in range(4):
                        tile = src[z * 4 + h, first + k]
                        if out is near:
                            for g in range(near.shape[0]):
                                near[g, z, :, column : column + 128] = tile
                        else:
                            far[z, :, column : column + 128] = tile
                    column += 128
            first += count


def own_kernel(pos, grid, mesh, out):
    rows = grid.shape[1]
    out[:rows, :] = grid[pos[2]]
    out[rows:, :] = mesh[pos[2]]


class Chunk:
    def __init__(self, widths):
        self.starts, self.widths, at = [], widths, 0
        for width in widths:
            self.starts.append(at)
            at += width

    def copies(self, k, dst, mine, theirs, core, sems):
        start, width = self.starts[k], self.widths[k]
        made = []
        for z in range(4):
            for n, (src, half) in enumerate(((mine, core), (theirs, 1 - core))):
                made.append(
                    pltpu.make_async_copy(
                        src.at[:, z, :, pl.ds(start, width)],
                        dst.at[z, :, half],
                        sems.at[z * 2 + n],
                    )
                )
        return made


CHUNK_A = Chunk((512, 512, 512))
CHUNK_B = Chunk((512,) * 5 + (2048,) * 2 + (512,) * 4)


def weight_scratch(chunk, members):
    return [pltpu.VMEM((4, 16, 2, 8, chunk.widths[m]), BF16) for m in members] + [
        pltpu.SemaphoreType.DMA((len(members), 8))
    ]


class Weights:
    def __init__(self, chunk, members, pos, mine, theirs, buffers, sems):
        core = pos[1]
        self.buffers = buffers
        self.made = [
            chunk.copies(m, buffers[n], mine, theirs, core, sems.at[n])
            for n, m in enumerate(members)
        ]
        for group in self.made:
            for copy in group:
                copy.start()

    def get(self, n):
        for copy in self.made[n]:
            copy.wait()
        buffer = self.buffers[n]
        return buffer.reshape(D, buffer.shape[-1])[...]


def softmax_mix(queries, keys, values, dead):
    scores = jnp.where(dead, -1e30, mm_t(queries, keys))
    weights = jnp.exp(scores - jnp.max(scores, axis=-1, keepdims=True))
    weights = weights * (1.0 / jnp.sum(weights, axis=-1, keepdims=True))
    return mm(weights.astype(BF16), values)


def two_heads(queries, keys, values, dead):
    first = lax.broadcasted_iota(jnp.int32, queries.shape, 1) < HEAD_DIM
    zero = jnp.zeros_like(queries)
    low = softmax_mix(jnp.where(first, queries, zero), keys, values, dead)
    high = softmax_mix(jnp.where(first, zero, queries), keys, values, dead)
    return jnp.where(first, low, high).astype(BF16)


def inputs_kernel(
    pos, x0, x1, x2, x3, mine, theirs, out0, out1, out2, out3, grid, mesh, staged, wk, wv, wq, sems
):
    weights = Weights(CHUNK_A, (0, 1, 2), pos, mine, theirs, (wk, wv, wq), sems)
    head = pos[2]
    rows, half = grid.shape[1], mesh.shape[1] // 2
    for k, part in enumerate((x0, x1, x2, x3)):
        grid[head ^ k] = part[:rows, :]
        mesh[head ^ k] = part[rows:, :]
    grid_norm = normalize(wide(grid))
    mesh_norm = normalize(wide(mesh))
    keys = mm(grid_norm, weights.get(0)).astype(BF16)
    for j in range(4):
        staged[j, :rows, :PAIR] = keys[:, j * PAIR : (j + 1) * PAIR]
    values = mm(grid_norm, weights.get(1)).astype(BF16)
    for j in range(4):
        staged[j, :rows, PAIR:] = values[:, j * PAIR : (j + 1) * PAIR]
    queries = (mm(mesh_norm, weights.get(2)) * SCALE).astype(BF16)
    for j in range(4):
        staged[j, rows:, :PAIR] = queries[:half, j * PAIR : (j + 1) * PAIR]
        staged[j, rows:, PAIR:] = queries[half:, j * PAIR : (j + 1) * PAIR]
    for k, out in enumerate((out0, out1, out2, out3)):
        out[...] = staged[head ^ k]


def arrange_kernel(pos, x0, x1, x2, x3, own, last, first):
    head = pos[2]
    for k, part in enumerate((x0, x1, x2, x3)):
        own[head ^ k] = part[...]
    last[...] = own[2:, :256, :]
    first[...] = own[:2, :256, :]


def encode_kernel(pos, blocks, count, own, before, after, out, tiles, picked):
    rows = own.shape[1] - 32
    for j in range(2):
        for k in range(2):
            part = slice(k * TILE, (k + 1) * TILE)
            tiles[j * 2 + k] = before[j, part]
            tiles[12 + j * 2 + k] = after[j, part]
    for j in range(4):
        for k in range(rows // TILE):
            tiles[4 + j * 2 + k] = own[j, k * TILE : (k + 1) * TILE]
    start = pos[0] * 8 - 4
    slots = blocks.shape[1]
    column = lax.broadcasted_iota(jnp.int32, (TILE, slots * TILE), 1)
    for m in range(2):
        for s in range(slots):
            index = jnp.clip(blocks[m, s] - start, 0, 15)
            picked[s * TILE : (s + 1) * TILE, :] = tiles[index]
        queries = jnp.concatenate(
            [
                own[2 * m + g, rows:, side * PAIR : (side + 1) * PAIR]
                for g in range(2)
                for side in range(2)
            ],
            axis=0,
        )
        mixed = two_heads(queries, picked[:, :PAIR], picked[:, PAIR:], column >= count[m] * TILE)
        out[2 * m] = mixed[:64]
        out[2 * m + 1] = mixed[64:]


def first_kernel(pos, encoded, mesh, mine, theirs, qkv, kept, wo, wq, wk, wv, sems):
    weights = Weights(CHUNK_B, (0, 1, 2, 3), pos, mine, theirs, (wo, wq, wk, wv), sems)
    update = mm_t(wide(encoded), weights.get(0))
    mesh_one = (wide(mesh).astype(F32) + update).astype(BF16)
    kept[...] = mesh_one
    norm_one = normalize(mesh_one)
    for n, scaling in enumerate((SCALE, 1.0, 1.0)):
        part = (mm(norm_one, weights.get(1 + n)) * scaling).astype(BF16)
        for j in range(4):
            qkv[j, :, n * PAIR : (n + 1) * PAIR] = part[:, j * PAIR : (j + 1) * PAIR]


def window_kernel(pos, offsets, own, before, after, out, tiles, picked):
    for j in range(4):
        half = slice((j % 2) * 64, (j % 2) * 64 + 64)
        tiles[j // 2, half] = before[j]
        tiles[2 + j // 2, half] = own[j, :, PAIR:]
        tiles[4 + j // 2, half] = after[j]
    slots = offsets.shape[1]
    slot = lax.broadcasted_iota(jnp.int32, (TILE, slots * TILE), 1) // TILE
    for m in range(2):
        alive = jnp.zeros((TILE, slots * TILE), jnp.int32)
        for s in range(slots):
            offset = offsets[m, s]
            picked[s * TILE : (s + 1) * TILE, :] = tiles[jnp.clip(m + 2 + offset, 0, 5)]
            reached = pos[0] * 2 + m + offset
            live = jnp.where((reached >= 0) & (reached < pos[3]), 1, 0)
            alive = jnp.where(slot == s, live, alive)
        queries = jnp.concatenate([own[2 * m, :, :PAIR], own[2 * m + 1, :, :PAIR]], axis=0)
        mixed = two_heads(queries, picked[:, :PAIR], picked[:, PAIR:], alive == 0)
        out[2 * m] = mixed[:64]
        out[2 * m + 1] = mixed[64:]


def second_kernel(
    pos, windowed, kept, mine, theirs, mesh_out, kv, wo, up, down, wk, wv, sems
):
    weights = Weights(CHUNK_B, (4, 5, 6, 7, 8), pos, mine, theirs, (wo, up, down, wk, wv), sems)
    update = mm_t(wide(windowed), weights.get(0))
    mesh_two = (kept[...].astype(F32) + update).astype(BF16)
    hidden = mm(normalize(mesh_two), weights.get(1))
    hidden = (0.5 * hidden * (1.0 + lax.erf(hidden * (2.0**-0.5)))).astype(BF16)
    result = (mesh_two.astype(F32) + mm_t(hidden, weights.get(2))).astype(BF16)
    for j in range(4):
        mesh_out[j] = result[:, j * 256 : (j + 1) * 256]
    norm_three = normalize(result)
    keys = mm(norm_three, weights.get(3)).astype(BF16)
    values = mm(norm_three, weights.get(4)).astype(BF16)
    for g in range(4):
        kv[g, :, :512] = keys
        kv[g, :, 512:] = values


def queries_kernel(pos, grid, mine, theirs, out, wq, sems):
    weights = Weights(CHUNK_B, (9,), pos, mine, theirs, (wq,), sems)
    out[...] = (mm(normalize(wide(grid)), weights.get(0)) * SCALE).astype(BF16)


def decode_kernel(pos, blocks, count, grid, queries, own, before, after, mine, theirs, out, wo,
                  tiles, picked, sems):
    weights = Weights(CHUNK_B, (10,), pos, mine, theirs, (wo,), sems)
    tiles[0] = before[...]
    for j in range(4):
        half = slice((j % 2) * 64, (j % 2) * 64 + 64)
        tiles[1 + j // 2, half] = own[j]
    tiles[3] = after[...]
    start = pos[0] * 2 - 1
    slots = blocks.shape[1]
    column = lax.broadcasted_iota(jnp.int32, (TILE, slots * TILE), 1)
    mixtures = []
    for t in range(2):
        row = pos[2] * 2 + t
        for s in range(slots):
            index = jnp.clip(blocks[row, s] - start, 0, 3)
            picked[s * TILE : (s + 1) * TILE, :] = tiles[index]
        dead = column >= count[row] * TILE
        mixtures.append(
            jnp.concatenate(
                [
                    two_heads(
                        queries[t * TILE : (t + 1) * TILE, j * PAIR : (j + 1) * PAIR],
                        picked[:, j * PAIR : (j + 1) * PAIR],
                        picked[:, 512 + j * PAIR : 512 + (j + 1) * PAIR],
                        dead,
                    )
                    for j in range(4)
                ],
                axis=1,
            )
        )
    decoded = jnp.concatenate(mixtures, axis=0)
    result = (wide(grid).astype(F32) + mm_t(decoded, weights.get(0))).astype(BF16)
    for j in range(4):
        out[j] = result[:, j * 256 : (j + 1) * 256]


def exchange(x):
    return lax.all_to_all(x, "heads", 0, 0, tiled=True)


def halo(last, first):
    size = lax.axis_size(NODES)
    up = [(i, i + 1) for i in range(size - 1)]
    down = [(j, i) for i, j in up]
    return lax.ppermute(last, NODES, up), lax.ppermute(first, NODES, down)


def after_it(x, other):
    return lax.optimization_barrier((x, other))[0]


def in_hbm(x):
    return pltpu.with_memory_space_constraint(x, pltpu.HBM)


def over_cores(x):
    return lax.ppermute(x, "core", [(0, 1), (1, 0)])


def trade(parts):
    out = [parts[0]]
    for k in range(1, 4):
        out.append(lax.ppermute(parts[k], "heads", [(i, i ^ k) for i in range(4)]))
    return out


def pack(sources):
    (tiles,) = call(
        pack_kernel, [(16, 20, 8, 128)], [in_vmem()] * len(sources), room=56
    )(*sources)
    return tiles


def over_plane(x):
    return lax.all_to_all(x, ("y", "x"), 0, 0, tiled=True)


def local(
    grid_state,
    mesh_state,
    encoder_query,
    encoder_key,
    encoder_value,
    encoder_output,
    window_query,
    window_key,
    window_value,
    window_output,
    expand_weight,
    shrink_weight,
    decoder_query,
    decoder_key,
    decoder_value,
    decoder_output,
    encoder_blocks,
    encoder_count,
    window_offsets,
    decoder_blocks,
    decoder_count,
):
    position = lax.axis_index(NODES)
    mesh_tiles = lax.axis_size(NODES) * 2
    pos = jnp.stack(
        [position, lax.axis_index("core"), lax.axis_index("heads"), jnp.int32(mesh_tiles),
         lax.axis_index("zh")]
    ).astype(jnp.int32)

    counts = ((1, 1, 1), (1, 1, 1, 1, 1, 4, 4, 1, 1, 1, 1))
    tiles = pack(
        (
            encoder_key, encoder_value, encoder_query, encoder_output.T, window_query, window_key,
            window_value, window_output.T, expand_weight, shrink_weight.T, decoder_key,
            decoder_value, decoder_query, decoder_output.T,
        )
    )
    tiles = lax.all_to_all(tiles, ("zh", "heads"), 0, 0, tiled=True)
    copies_a, rows = call(
        functools.partial(regroup_kernel, counts),
        [(16, 4, 8, 1536), (4, 8, 8704)],
        [in_vmem()],
    )(tiles)
    mine = lax.all_gather(rows, ("y", "x"))
    mine_a = over_plane(copies_a)
    theirs_a = over_cores(mine_a)


    head = lax.axis_index("heads")
    grid_parts, mesh_parts = grid_state.reshape(4, 256, 256), mesh_state.reshape(4, 64, 256)
    both = call(
        own_kernel, [(320, 256)], [in_smem(), in_vmem(), in_vmem()], room=8
    )(pos, grid_parts, mesh_parts)
    both += tuple(
        jnp.concatenate(
            [
                lax.dynamic_index_in_dim(after_it(x, copies_a), head ^ k, 0, False)
                for x in (grid_parts, mesh_parts)
            ]
        )
        for k in range(1, 4)
    )
    *sent, grid, mesh = call(
        inputs_kernel,
        [(288, 256)] * 4 + [(4, 256, 256), (4, 64, 256)],
        [in_smem()] + [in_vmem()] * 4 + [in_any(), in_any()],
        [pltpu.VMEM((4, 288, 256), BF16)] + weight_scratch(CHUNK_A, (0, 1, 2)),
        room=16,
    )(pos, *trade(both), mine_a, theirs_a)
    own, last, first = call(
        arrange_kernel,
        [(4, 288, 256), (2, 256, 256), (2, 256, 256)],
        [in_smem()] + [in_vmem()] * 4,
        room=8,
    )(pos, *trade(sent))
    before, after = halo(last, first)
    (sent,) = call(
        encode_kernel,
        [(4, 64, 128)],
        [in_smem()] * 3 + [in_vmem()] * 3,
        [pltpu.VMEM((16, TILE, 256), BF16), pltpu.VMEM((8 * TILE, 256), BF16)],
    )(pos, encoder_blocks, encoder_count, own, before, after)
    encoded = exchange(sent)
    mine = after_it(mine, encoded)
    theirs_b = over_cores(mine[:, :, :, :2048])
    theirs = over_cores(mine)
    mine, late = in_hbm(mine), in_hbm(theirs)
    sent, kept = call(
        first_kernel,
        [(4, 64, 384), (64, D)],
        [in_smem(), in_vmem(), in_vmem(), in_any(), in_any()],
        weight_scratch(CHUNK_B, (0, 1, 2, 3)),
        room=16,
    )(pos, encoded, mesh, mine, theirs_b)
    own = exchange(sent)
    side = own[:, :, PAIR:]
    before, after = halo(side, side)
    (sent,) = call(
        window_kernel,
        [(4, 64, 128)],
        [in_smem()] * 2 + [in_vmem()] * 3,
        [pltpu.VMEM((6, TILE, 256), BF16), pltpu.VMEM((4 * TILE, 256), BF16)],
    )(pos, window_offsets, own, before, after)
    windowed = exchange(sent)
    sent, spread = call(
        second_kernel,
        [(4, 64, 256), (4, 64, D)],
        [in_smem(), in_vmem(), in_vmem()] + [in_any()] * 2,
        weight_scratch(CHUNK_B, (4, 5, 6, 7, 8)),
        room=24,
    )(pos, windowed, kept, mine, theirs)
    own = exchange(spread)
    before, after = halo(own[2:].reshape(TILE, D), own[:2].reshape(TILE, D))
    mesh_out = exchange(sent).reshape(256, 256)
    (queries,) = call(
        queries_kernel,
        [(256, 512)],
        [in_smem(), in_vmem()] + [in_any()] * 2,
        weight_scratch(CHUNK_B, (9,)),
        room=12,
    )(pos, grid, mine, late)
    last = weight_scratch(CHUNK_B, (10,))
    (sent,) = call(
        decode_kernel,
        [(4, 256, 256)],
        [in_smem()] * 3 + [in_vmem()] * 5 + [in_any()] * 2,
        last[:-1]
        + [pltpu.VMEM((4, TILE, D), BF16), pltpu.VMEM((3 * TILE, D), BF16), last[-1]],
        room=16,
    )(pos, decoder_blocks, decoder_count, grid, queries, own, before, after, mine, late)
    grid_out = exchange(sent).reshape(1024, 256)
    return grid_out, mesh_out


def solution(mesh):
    sizes = (4, 4, 4, 2)
    fine = Mesh(mesh.devices.reshape(*sizes, mesh.devices.shape[1]), (*NODES, "heads"))
    both, flipped = P(NODES, "heads"), P("heads", NODES)
    in_specs = (
        both, both, both, both, both, flipped, both, both, both, flipped, both, flipped,
        both, both, both, flipped,
        P(NODES, None), P(NODES), P(NODES, None), P(NODES, None), P(NODES),
    )
    return jax.shard_map(
        local, mesh=fine, in_specs=in_specs, out_specs=(both, both), check_vma=False
    )
```

```python
import functools

import jax
import jax.numpy as jnp
from jax import lax
from jax.experimental import pallas as pl
from jax.experimental.pallas import tpu as pltpu
from jax.sharding import Mesh
from jax.sharding import PartitionSpec as P


HEAD_DIM = 64
TILE = 128
PAIR = 2 * HEAD_DIM
D = 1024
SCALE = HEAD_DIM ** (-0.5)
EPSILON = 1e-05
NODES = ("zh", "y", "x", "core")
F32 = jnp.float32
BF16 = jnp.bfloat16


def in_vmem():
    return pl.BlockSpec(memory_space=pltpu.VMEM)


def in_smem():
    return pl.BlockSpec(memory_space=pltpu.SMEM)


def in_any():
    return pl.BlockSpec(memory_space=pltpu.HBM)


def call(kernel, outs, specs, scratch=(), flops=1 << 28, room=12):
    return pl.pallas_call(
        kernel,
        out_shape=tuple(jax.ShapeDtypeStruct(shape, BF16) for shape in outs),
        in_specs=list(specs),
        out_specs=tuple(in_vmem() for _ in outs),
        scratch_shapes=list(scratch),
        compiler_params=pltpu.CompilerParams(vmem_limit_bytes=room << 20),
        cost_estimate=pl.CostEstimate(flops=flops, bytes_accessed=1 << 20, transcendentals=0),
    )


def mm(a, b):
    return jnp.dot(a, b, preferred_element_type=F32)


def mm_t(a, b):
    return lax.dot_general(a, b, (((1,), (1,)), ((), ())), preferred_element_type=F32)


def normalize(values):
    values = values.astype(F32)
    average = jnp.mean(values, axis=-1, keepdims=True)
    centred = values - average
    spread = jnp.mean(centred * centred, axis=-1, keepdims=True)
    return (centred * lax.rsqrt(spread + EPSILON)).astype(BF16)


def wide(ref):
    return jnp.concatenate([ref[k] for k in range(ref.shape[0])], axis=-1)


def pack_kernel(*refs):
    *sources, out = refs
    t = 0
    for source in sources:
        whole = source[...]
        for k in range(0, whole.shape[1], 128):
            for g in range(out.shape[0]):
                out[g, t] = whole[:, k : k + 128]
            t += 1


def regroup_kernel(counts, src, near, far):
    first = 0
    for out, members in zip((near, far), counts):
        column = 0
        for count in members:
            for h in range(4):
                for k in range(count):
                    for z in range(4):
                        tile = src[z * 4 + h, first + k]
                        if out is near:
                            for g in range(near.shape[0]):
                                near[g, z, :, column : column + 128] = tile
                        else:
                            far[z, :, column : column + 128] = tile
                    column += 128
            first += count


def own_kernel(pos, grid, mesh, out):
    rows = grid.shape[1]
    out[:rows, :] = grid[pos[2]]
    out[rows:, :] = mesh[pos[2]]


class Chunk:
    def __init__(self, widths):
        self.starts, self.widths, at = [], widths, 0
        for width in widths:
            self.starts.append(at)
            at += width

    def copies(self, k, dst, mine, theirs, core, sems):
        start, width = self.starts[k], self.widths[k]
        made = []
        for z in range(4):
            for n, (src, half) in enumerate(((mine, core), (theirs, 1 - core))):
                made.append(
                    pltpu.make_async_copy(
                        src.at[:, z, :, pl.ds(start, width)],
                        dst.at[z, :, half],
                        sems.at[z * 2 + n],
                    )
                )
        return made


CHUNK_A = Chunk((512, 512, 512))
CHUNK_B = Chunk((512,) * 5 + (2048,) * 2 + (512,) * 4)


def weight_scratch(chunk, members):
    return [pltpu.VMEM((4, 16, 2, 8, chunk.widths[m]), BF16) for m in members] + [
        pltpu.SemaphoreType.DMA((len(members), 8))
    ]


class Weights:
    def __init__(self, chunk, members, pos, mine, theirs, buffers, sems):
        core = pos[1]
        self.buffers = buffers
        self.made = [
            chunk.copies(m, buffers[n], mine, theirs, core, sems.at[n])
            for n, m in enumerate(members)
        ]
        for group in self.made:
            for copy in group:
                copy.start()

    def get(self, n):
        for copy in self.made[n]:
            copy.wait()
        buffer = self.buffers[n]
        return buffer.reshape(D, buffer.shape[-1])[...]


def softmax_mix(queries, keys, values, dead):
    scores = jnp.where(dead, -1e30, mm_t(queries, keys))
    weights = jnp.exp(scores - jnp.max(scores, axis=-1, keepdims=True))
    weights = weights * (1.0 / jnp.sum(weights, axis=-1, keepdims=True))
    return mm(weights.astype(BF16), values)


def two_heads(queries, keys, values, dead):
    first = lax.broadcasted_iota(jnp.int32, queries.shape, 1) < HEAD_DIM
    zero = jnp.zeros_like(queries)
    stacked = jnp.concatenate(
        [jnp.where(first, queries, zero), jnp.where(first, zero, queries)], axis=0
    )
    mixed = softmax_mix(stacked, keys, values, dead)
    rows = queries.shape[0]
    return jnp.where(first, mixed[:rows], mixed[rows:]).astype(BF16)


def inputs_kernel(
    pos, x0, x1, x2, x3, mine, theirs, staged, grid, mesh, wk, wv, wq, sems
):
    weights = Weights(CHUNK_A, (0, 1, 2), pos, mine, theirs, (wk, wv, wq), sems)
    head = pos[2]
    rows, half = grid.shape[1], mesh.shape[1] // 2
    for k, part in enumerate((x0, x1, x2, x3)):
        grid[head ^ k] = part[:rows, :]
        mesh[head ^ k] = part[rows:, :]
    grid_norm = normalize(wide(grid))
    mesh_norm = normalize(wide(mesh))
    keys = mm(grid_norm, weights.get(0)).astype(BF16)
    for j in range(4):
        staged[j, :rows, :PAIR] = keys[:, j * PAIR : (j + 1) * PAIR]
    values = mm(grid_norm, weights.get(1)).astype(BF16)
    for j in range(4):
        staged[j, :rows, PAIR:] = values[:, j * PAIR : (j + 1) * PAIR]
    queries = (mm(mesh_norm, weights.get(2)) * SCALE).astype(BF16)
    for j in range(4):
        staged[j, rows:, :PAIR] = queries[:half, j * PAIR : (j + 1) * PAIR]
        staged[j, rows:, PAIR:] = queries[half:, j * PAIR : (j + 1) * PAIR]


def encode_kernel(pos, blocks, count, own, before, after, out, tiles, picked):
    rows = own.shape[1] - 32
    for j in range(2):
        for k in range(2):
            part = slice(k * TILE, (k + 1) * TILE)
            tiles[j * 2 + k] = before[j, part]
            tiles[12 + j * 2 + k] = after[j, part]
    for j in range(4):
        for k in range(rows // TILE):
            tiles[4 + j * 2 + k] = own[j, k * TILE : (k + 1) * TILE]
    start = pos[0] * 8 - 4
    slots = blocks.shape[1]
    column = lax.broadcasted_iota(jnp.int32, (2 * TILE, slots * TILE), 1)
    for m in range(2):
        for s in range(slots):
            index = jnp.clip(blocks[m, s] - start, 0, 15)
            picked[s * TILE : (s + 1) * TILE, :] = tiles[index]
        queries = jnp.concatenate(
            [
                own[2 * m + g, rows:, side * PAIR : (side + 1) * PAIR]
                for g in range(2)
                for side in range(2)
            ],
            axis=0,
        )
        mixed = two_heads(queries, picked[:, :PAIR], picked[:, PAIR:], column >= count[m] * TILE)
        out[2 * m] = mixed[:64]
        out[2 * m + 1] = mixed[64:]


def first_kernel(pos, encoded, mesh, mine, theirs, qkv, kept, wo, wq, wk, wv, sems):
    weights = Weights(CHUNK_B, (0, 1, 2, 3), pos, mine, theirs, (wo, wq, wk, wv), sems)
    update = mm_t(wide(encoded), weights.get(0))
    mesh_one = (wide(mesh).astype(F32) + update).astype(BF16)
    kept[...] = mesh_one
    norm_one = normalize(mesh_one)
    for n, scaling in enumerate((SCALE, 1.0, 1.0)):
        part = (mm(norm_one, weights.get(1 + n)) * scaling).astype(BF16)
        for j in range(4):
            qkv[j, :, n * PAIR : (n + 1) * PAIR] = part[:, j * PAIR : (j + 1) * PAIR]


def window_kernel(pos, offsets, own, before, after, out, tiles, picked):
    for j in range(4):
        half = slice((j % 2) * 64, (j % 2) * 64 + 64)
        tiles[j // 2, half] = before[j]
        tiles[2 + j // 2, half] = own[j, :, PAIR:]
        tiles[4 + j // 2, half] = after[j]
    slots = offsets.shape[1]
    slot = lax.broadcasted_iota(jnp.int32, (2 * TILE, slots * TILE), 1) // TILE
    for m in range(2):
        alive = jnp.zeros((2 * TILE, slots * TILE), jnp.int32)
        for s in range(slots):
            offset = offsets[m, s]
            picked[s * TILE : (s + 1) * TILE, :] = tiles[jnp.clip(m + 2 + offset, 0, 5)]
            reached = pos[0] * 2 + m + offset
            live = jnp.where((reached >= 0) & (reached < pos[3]), 1, 0)
            alive = jnp.where(slot == s, live, alive)
        queries = jnp.concatenate([own[2 * m, :, :PAIR], own[2 * m + 1, :, :PAIR]], axis=0)
        mixed = two_heads(queries, picked[:, :PAIR], picked[:, PAIR:], alive == 0)
        out[2 * m] = mixed[:64]
        out[2 * m + 1] = mixed[64:]


def second_kernel(
    pos, windowed, kept, mine, theirs, mesh_out, kv, wo, up, down, wk, wv, sems
):
    weights = Weights(CHUNK_B, (4, 5, 6, 7, 8), pos, mine, theirs, (wo, up, down, wk, wv), sems)
    update = mm_t(wide(windowed), weights.get(0))
    mesh_two = (kept[...].astype(F32) + update).astype(BF16)
    hidden = mm(normalize(mesh_two), weights.get(1))
    hidden = (0.5 * hidden * (1.0 + lax.erf(hidden * (2.0**-0.5)))).astype(BF16)
    result = (mesh_two.astype(F32) + mm_t(hidden, weights.get(2))).astype(BF16)
    for j in range(4):
        mesh_out[j] = result[:, j * 256 : (j + 1) * 256]
    norm_three = normalize(result)
    keys = mm(norm_three, weights.get(3)).astype(BF16)
    values = mm(norm_three, weights.get(4)).astype(BF16)
    kv[:, :512] = keys
    kv[:, 512:] = values


def queries_kernel(pos, grid, mine, theirs, out, wq, sems):
    weights = Weights(CHUNK_B, (9,), pos, mine, theirs, (wq,), sems)
    out[...] = (mm(normalize(wide(grid)), weights.get(0)) * SCALE).astype(BF16)


def decode_kernel(pos, blocks, count, grid, queries, own, before, after, mine, theirs, out, wo,
                  tiles, picked, sems):
    weights = Weights(CHUNK_B, (10,), pos, mine, theirs, (wo,), sems)
    tiles[0] = before[...]
    for j in range(4):
        half = slice((j % 2) * 64, (j % 2) * 64 + 64)
        tiles[1 + j // 2, half] = own[j]
    tiles[3] = after[...]
    start = pos[0] * 2 - 1
    slots = blocks.shape[1]
    column = lax.broadcasted_iota(jnp.int32, (2 * TILE, slots * TILE), 1)
    mixtures = []
    for t in range(2):
        row = pos[2] * 2 + t
        for s in range(slots):
            index = jnp.clip(blocks[row, s] - start, 0, 3)
            picked[s * TILE : (s + 1) * TILE, :] = tiles[index]
        dead = column >= count[row] * TILE
        mixtures.append(
            jnp.concatenate(
                [
                    two_heads(
                        queries[t * TILE : (t + 1) * TILE, j * PAIR : (j + 1) * PAIR],
                        picked[:, j * PAIR : (j + 1) * PAIR],
                        picked[:, 512 + j * PAIR : 512 + (j + 1) * PAIR],
                        dead,
                    )
                    for j in range(4)
                ],
                axis=1,
            )
        )
    decoded = jnp.concatenate(mixtures, axis=0)
    result = (wide(grid).astype(F32) + mm_t(decoded, weights.get(0))).astype(BF16)
    for j in range(4):
        out[j] = result[:, j * 256 : (j + 1) * 256]


def exchange(x):
    return lax.all_to_all(x, "heads", 0, 0, tiled=True)


def halo(last, first):
    size = lax.axis_size(NODES)
    up = [(i, i + 1) for i in range(size - 1)]
    down = [(j, i) for i, j in up]
    return lax.ppermute(last, NODES, up), lax.ppermute(first, NODES, down)


def after_it(x, other):
    return lax.optimization_barrier((x, other))[0]


def in_hbm(x):
    return pltpu.with_memory_space_constraint(x, pltpu.HBM)


def over_cores(x):
    return lax.ppermute(x, "core", [(0, 1), (1, 0)])


def trade(parts):
    out = [parts[0]]
    for k in range(1, 4):
        out.append(lax.ppermute(parts[k], "heads", [(i, i ^ k) for i in range(4)]))
    return out


def pack(sources):
    (tiles,) = call(
        pack_kernel, [(16, 20, 8, 128)], [in_vmem()] * len(sources), room=56
    )(*sources)
    return tiles


def over_plane(x):
    return lax.all_to_all(x, ("y", "x"), 0, 0, tiled=True)


def local(
    grid_state,
    mesh_state,
    encoder_query,
    encoder_key,
    encoder_value,
    encoder_output,
    window_query,
    window_key,
    window_value,
    window_output,
    expand_weight,
    shrink_weight,
    decoder_query,
    decoder_key,
    decoder_value,
    decoder_output,
    encoder_blocks,
    encoder_count,
    window_offsets,
    decoder_blocks,
    decoder_count,
):
    position = lax.axis_index(NODES)
    mesh_tiles = lax.axis_size(NODES) * 2
    pos = jnp.stack(
        [position, lax.axis_index("core"), lax.axis_index("heads"), jnp.int32(mesh_tiles),
         lax.axis_index("zh")]
    ).astype(jnp.int32)

    counts = ((1, 1, 1), (1, 1, 1, 1, 1, 4, 4, 1, 1, 1, 1))
    tiles = pack(
        (
            encoder_key, encoder_value, encoder_query, encoder_output.T, window_query, window_key,
            window_value, window_output.T, expand_weight, shrink_weight.T, decoder_key,
            decoder_value, decoder_query, decoder_output.T,
        )
    )
    tiles = lax.all_to_all(tiles, ("zh", "heads"), 0, 0, tiled=True)
    copies_a, rows = call(
        functools.partial(regroup_kernel, counts),
        [(16, 4, 8, 1536), (4, 8, 8704)],
        [in_vmem()],
    )(tiles)
    mine = lax.all_gather(rows, ("y", "x"))
    mine_a = over_plane(copies_a)
    theirs_a = over_cores(mine_a)


    head = lax.axis_index("heads")
    grid_parts, mesh_parts = grid_state.reshape(4, 256, 256), mesh_state.reshape(4, 64, 256)
    both = call(
        own_kernel, [(320, 256)], [in_smem(), in_vmem(), in_vmem()], room=8
    )(pos, grid_parts, mesh_parts)
    both += tuple(
        jnp.concatenate(
            [
                lax.dynamic_index_in_dim(after_it(x, copies_a), head ^ k, 0, False)
                for x in (grid_parts, mesh_parts)
            ]
        )
        for k in range(1, 4)
    )
    sent, grid, mesh = call(
        inputs_kernel,
        [(4, 288, 256), (4, 256, 256), (4, 64, 256)],
        [in_smem()] + [in_vmem()] * 4 + [in_any(), in_any()],
        weight_scratch(CHUNK_A, (0, 1, 2)),
        room=16,
    )(pos, *trade(both), mine_a, theirs_a)
    own = exchange(sent)
    before, after = halo(own[2:, :256], own[:2, :256])
    (sent,) = call(
        encode_kernel,
        [(4, 64, 128)],
        [in_smem()] * 3 + [in_vmem()] * 3,
        [pltpu.VMEM((16, TILE, 256), BF16), pltpu.VMEM((8 * TILE, 256), BF16)],
    )(pos, encoder_blocks, encoder_count, own, before, after)
    encoded = exchange(sent)
    mine = after_it(mine, sent)
    theirs_b = over_cores(mine[:, :, :, :2048])
    theirs = over_cores(mine)
    mine, late = in_hbm(mine), in_hbm(theirs)
    sent, kept = call(
        first_kernel,
        [(4, 64, 384), (64, D)],
        [in_smem(), in_vmem(), in_vmem(), in_any(), in_any()],
        weight_scratch(CHUNK_B, (0, 1, 2, 3)),
        room=16,
    )(pos, encoded, mesh, mine, theirs_b)
    own = exchange(sent)
    side = own[:, :, PAIR:]
    before, after = halo(side, side)
    (sent,) = call(
        window_kernel,
        [(4, 64, 128)],
        [in_smem()] * 2 + [in_vmem()] * 3,
        [pltpu.VMEM((6, TILE, 256), BF16), pltpu.VMEM((4 * TILE, 256), BF16)],
    )(pos, window_offsets, own, before, after)
    windowed = exchange(sent)
    sent, spread = call(
        second_kernel,
        [(4, 64, 256), (64, D)],
        [in_smem(), in_vmem(), in_vmem()] + [in_any()] * 2,
        weight_scratch(CHUNK_B, (4, 5, 6, 7, 8)),
        room=24,
    )(pos, windowed, kept, mine, theirs)
    own = lax.all_gather(spread, "heads")
    before, after = halo(own[2:].reshape(TILE, D), own[:2].reshape(TILE, D))
    mesh_out = exchange(sent).reshape(256, 256)
    (queries,) = call(
        queries_kernel,
        [(256, 512)],
        [in_smem(), in_vmem()] + [in_any()] * 2,
        weight_scratch(CHUNK_B, (9,)),
        room=12,
    )(pos, grid, mine, late)
    last = weight_scratch(CHUNK_B, (10,))
    (sent,) = call(
        decode_kernel,
        [(4, 256, 256)],
        [in_smem()] * 3 + [in_vmem()] * 5 + [in_any()] * 2,
        last[:-1]
        + [pltpu.VMEM((4, TILE, D), BF16), pltpu.VMEM((3 * TILE, D), BF16), last[-1]],
        room=16,
    )(pos, decoder_blocks, decoder_count, grid, queries, own, before, after, mine, late)
    grid_out = exchange(sent).reshape(1024, 256)
    return grid_out, mesh_out


def solution(mesh):
    sizes = (4, 4, 4, 2)
    fine = Mesh(mesh.devices.reshape(*sizes, mesh.devices.shape[1]), (*NODES, "heads"))
    both, flipped = P(NODES, "heads"), P("heads", NODES)
    in_specs = (
        both, both, both, both, both, flipped, both, both, both, flipped, both, flipped,
        both, both, both, flipped,
        P(NODES, None), P(NODES), P(NODES, None), P(NODES, None), P(NODES),
    )
    return jax.shard_map(
        local, mesh=fine, in_specs=in_specs, out_specs=(both, both), check_vma=False
    )
```

```python
import functools

import jax
import jax.numpy as jnp
from jax import lax
from jax.experimental import pallas as pl
from jax.experimental.pallas import tpu as pltpu
from jax.sharding import Mesh
from jax.sharding import PartitionSpec as P


HEAD_DIM = 64
TILE = 128
PAIR = 2 * HEAD_DIM
D = 1024
SCALE = HEAD_DIM ** (-0.5)
EPSILON = 1e-05
NODES = ("zh", "y", "x", "core")
F32 = jnp.float32
BF16 = jnp.bfloat16


def in_vmem():
    return pl.BlockSpec(memory_space=pltpu.VMEM)


def in_smem():
    return pl.BlockSpec(memory_space=pltpu.SMEM)


def in_any():
    return pl.BlockSpec(memory_space=pltpu.HBM)


def call(kernel, outs, specs, scratch=(), flops=1 << 28, room=12):
    return pl.pallas_call(
        kernel,
        out_shape=tuple(jax.ShapeDtypeStruct(shape, BF16) for shape in outs),
        in_specs=list(specs),
        out_specs=tuple(in_vmem() for _ in outs),
        scratch_shapes=list(scratch),
        compiler_params=pltpu.CompilerParams(vmem_limit_bytes=room << 20),
        cost_estimate=pl.CostEstimate(flops=flops, bytes_accessed=1 << 20, transcendentals=0),
    )


def mm(a, b):
    return jnp.dot(a, b, preferred_element_type=F32)


def mm_t(a, b):
    return lax.dot_general(a, b, (((1,), (1,)), ((), ())), preferred_element_type=F32)


def normalize(values):
    values = values.astype(F32)
    average = jnp.mean(values, axis=-1, keepdims=True)
    centred = values - average
    spread = jnp.mean(centred * centred, axis=-1, keepdims=True)
    return (centred * lax.rsqrt(spread + EPSILON)).astype(BF16)


def wide(ref):
    return jnp.concatenate([ref[k] for k in range(ref.shape[0])], axis=-1)


def pack_kernel(*refs):
    *sources, out = refs
    t = 0
    for source in sources:
        whole = source[...]
        for k in range(0, whole.shape[1], 128):
            for g in range(out.shape[0]):
                out[g, t] = whole[:, k : k + 128]
            t += 1


def regroup_kernel(counts, src, near, far):
    first = 0
    for out, members in zip((near, far), counts):
        column = 0
        for count in members:
            for h in range(4):
                for k in range(count):
                    for z in range(4):
                        tile = src[z * 4 + h, first + k]
                        if out is near:
                            for g in range(near.shape[0]):
                                near[g, z, :, column : column + 128] = tile
                        else:
                            far[z, :, column : column + 128] = tile
                    column += 128
            first += count


def own_kernel(pos, grid, mesh, out):
    rows = grid.shape[1]
    out[:rows, :] = grid[pos[2]]
    out[rows:, :] = mesh[pos[2]]


class Chunk:
    def __init__(self, widths):
        self.starts, self.widths, at = [], widths, 0
        for width in widths:
            self.starts.append(at)
            at += width

    def copies(self, k, dst, mine, theirs, core, sems):
        start, width = self.starts[k], self.widths[k]
        made = []
        for z in range(4):
            for n, (src, half) in enumerate(((mine, core), (theirs, 1 - core))):
                made.append(
                    pltpu.make_async_copy(
                        src.at[:, z, :, pl.ds(start, width)],
                        dst.at[z, :, half],
                        sems.at[z * 2 + n],
                    )
                )
        return made


CHUNK_A = Chunk((512, 512, 512))
CHUNK_B = Chunk((512,) * 5 + (2048,) * 2 + (512,) * 4)


def weight_scratch(chunk, members):
    return [pltpu.VMEM((4, 16, 2, 8, chunk.widths[m]), BF16) for m in members] + [
        pltpu.SemaphoreType.DMA((len(members), 8))
    ]


class Weights:
    def __init__(self, chunk, members, pos, mine, theirs, buffers, sems):
        core = pos[1]
        self.buffers = buffers
        self.made = [
            chunk.copies(m, buffers[n], mine, theirs, core, sems.at[n])
            for n, m in enumerate(members)
        ]
        for group in self.made:
            for copy in group:
                copy.start()

    def get(self, n):
        for copy in self.made[n]:
            copy.wait()
        buffer = self.buffers[n]
        return buffer.reshape(D, buffer.shape[-1])[...]


def softmax_mix(queries, keys, values, dead):
    scores = jnp.where(dead, -1e30, mm_t(queries, keys))
    weights = jnp.exp(scores - jnp.max(scores, axis=-1, keepdims=True))
    weights = weights * (1.0 / jnp.sum(weights, axis=-1, keepdims=True))
    return mm(weights.astype(BF16), values)


def two_heads(queries, keys, values, dead):
    first = lax.broadcasted_iota(jnp.int32, queries.shape, 1) < HEAD_DIM
    zero = jnp.zeros_like(queries)
    stacked = jnp.concatenate(
        [jnp.where(first, queries, zero), jnp.where(first, zero, queries)], axis=0
    )
    mixed = softmax_mix(stacked, keys, values, dead)
    rows = queries.shape[0]
    return jnp.where(first, mixed[:rows], mixed[rows:]).astype(BF16)


def inputs_kernel(
    pos, x0, x1, x2, x3, mine, theirs, staged, grid, mesh, wk, wv, wq, sems
):
    weights = Weights(CHUNK_A, (0, 1, 2), pos, mine, theirs, (wk, wv, wq), sems)
    head = pos[2]
    rows, half = grid.shape[1], mesh.shape[1] // 2
    for k, part in enumerate((x0, x1, x2, x3)):
        grid[head ^ k] = part[:rows, :]
        mesh[head ^ k] = part[rows:, :]
    grid_norm = normalize(wide(grid))
    mesh_norm = normalize(wide(mesh))
    keys = mm(grid_norm, weights.get(0)).astype(BF16)
    for j in range(4):
        staged[j, :rows, :PAIR] = keys[:, j * PAIR : (j + 1) * PAIR]
    values = mm(grid_norm, weights.get(1)).astype(BF16)
    for j in range(4):
        staged[j, :rows, PAIR:] = values[:, j * PAIR : (j + 1) * PAIR]
    queries = (mm(mesh_norm, weights.get(2)) * SCALE).astype(BF16)
    for j in range(4):
        staged[j, rows:, :PAIR] = queries[:half, j * PAIR : (j + 1) * PAIR]
        staged[j, rows:, PAIR:] = queries[half:, j * PAIR : (j + 1) * PAIR]


def encode_kernel(pos, blocks, count, own, before, after, out, tiles, picked):
    rows = own.shape[1] - 32
    for j in range(2):
        for k in range(2):
            part = slice(k * TILE, (k + 1) * TILE)
            tiles[j * 2 + k] = before[j, part]
            tiles[12 + j * 2 + k] = after[j, part]
    for j in range(4):
        for k in range(rows // TILE):
            tiles[4 + j * 2 + k] = own[j, k * TILE : (k + 1) * TILE]
    start = pos[0] * 8 - 4
    slots = blocks.shape[1]
    column = lax.broadcasted_iota(jnp.int32, (2 * TILE, slots * TILE), 1)
    for m in range(2):
        for s in range(slots):
            index = jnp.clip(blocks[m, s] - start, 0, 15)
            picked[s * TILE : (s + 1) * TILE, :] = tiles[index]
        queries = jnp.concatenate(
            [
                own[2 * m + g, rows:, side * PAIR : (side + 1) * PAIR]
                for g in range(2)
                for side in range(2)
            ],
            axis=0,
        )
        mixed = two_heads(queries, picked[:, :PAIR], picked[:, PAIR:], column >= count[m] * TILE)
        out[2 * m] = mixed[:64]
        out[2 * m + 1] = mixed[64:]


def first_kernel(pos, encoded, mesh, mine, theirs, qkv, kept, wo, wq, wk, wv, sems):
    weights = Weights(CHUNK_B, (0, 1, 2, 3), pos, mine, theirs, (wo, wq, wk, wv), sems)
    update = mm_t(wide(encoded), weights.get(0))
    mesh_one = (wide(mesh).astype(F32) + update).astype(BF16)
    kept[...] = mesh_one
    norm_one = normalize(mesh_one)
    for n, scaling in enumerate((SCALE, 1.0, 1.0)):
        part = (mm(norm_one, weights.get(1 + n)) * scaling).astype(BF16)
        for j in range(4):
            qkv[j, :, n * PAIR : (n + 1) * PAIR] = part[:, j * PAIR : (j + 1) * PAIR]


def window_kernel(pos, offsets, own, before, after, out, tiles, picked):
    for j in range(4):
        half = slice((j % 2) * 64, (j % 2) * 64 + 64)
        tiles[j // 2, half] = before[j]
        tiles[2 + j // 2, half] = own[j, :, PAIR:]
        tiles[4 + j // 2, half] = after[j]
    slots = offsets.shape[1]
    slot = lax.broadcasted_iota(jnp.int32, (2 * TILE, slots * TILE), 1) // TILE
    for m in range(2):
        alive = jnp.zeros((2 * TILE, slots * TILE), jnp.int32)
        for s in range(slots):
            offset = offsets[m, s]
            picked[s * TILE : (s + 1) * TILE, :] = tiles[jnp.clip(m + 2 + offset, 0, 5)]
            reached = pos[0] * 2 + m + offset
            live = jnp.where((reached >= 0) & (reached < pos[3]), 1, 0)
            alive = jnp.where(slot == s, live, alive)
        queries = jnp.concatenate([own[2 * m, :, :PAIR], own[2 * m + 1, :, :PAIR]], axis=0)
        mixed = two_heads(queries, picked[:, :PAIR], picked[:, PAIR:], alive == 0)
        out[2 * m] = mixed[:64]
        out[2 * m + 1] = mixed[64:]


def second_kernel(
    pos, windowed, kept, mine, theirs, mesh_out, kv, wo, up, down, wk, wv, sems
):
    weights = Weights(CHUNK_B, (4, 5, 6, 7, 8), pos, mine, theirs, (wo, up, down, wk, wv), sems)
    update = mm_t(wide(windowed), weights.get(0))
    mesh_two = (kept[...].astype(F32) + update).astype(BF16)
    hidden = mm(normalize(mesh_two), weights.get(1))
    hidden = (0.5 * hidden * (1.0 + lax.erf(hidden * (2.0**-0.5)))).astype(BF16)
    result = (mesh_two.astype(F32) + mm_t(hidden, weights.get(2))).astype(BF16)
    for j in range(4):
        mesh_out[j] = result[:, j * 256 : (j + 1) * 256]
    norm_three = normalize(result)
    keys = mm(norm_three, weights.get(3)).astype(BF16)
    values = mm(norm_three, weights.get(4)).astype(BF16)
    kv[:, :512] = keys
    kv[:, 512:] = values


def queries_kernel(pos, grid, mine, theirs, out, wq, sems):
    weights = Weights(CHUNK_B, (9,), pos, mine, theirs, (wq,), sems)
    out[...] = (mm(normalize(wide(grid)), weights.get(0)) * SCALE).astype(BF16)


def decode_kernel(pos, blocks, count, grid, queries, own, r0, r1, r2, r3, mine, theirs, out, wo,
                  tiles, sides, picked, sems):
    weights = Weights(CHUNK_B, (10,), pos, mine, theirs, (wo,), sems)
    for k, part in enumerate((r0, r1, r2, r3)):
        sides[pos[2] ^ k] = part[...]
    for j in range(4):
        half = slice((j % 2) * 64, (j % 2) * 64 + 64)
        tiles[1 + j // 2, half] = own[j]
        tiles[0 if j >= 2 else 3, half] = sides[j]
    start = pos[0] * 2 - 1
    slots = blocks.shape[1]
    column = lax.broadcasted_iota(jnp.int32, (2 * TILE, slots * TILE), 1)
    mixtures = []
    for t in range(2):
        row = pos[2] * 2 + t
        for s in range(slots):
            index = jnp.clip(blocks[row, s] - start, 0, 3)
            picked[s * TILE : (s + 1) * TILE, :] = tiles[index]
        dead = column >= count[row] * TILE
        mixtures.append(
            jnp.concatenate(
                [
                    two_heads(
                        queries[t * TILE : (t + 1) * TILE, j * PAIR : (j + 1) * PAIR],
                        picked[:, j * PAIR : (j + 1) * PAIR],
                        picked[:, 512 + j * PAIR : 512 + (j + 1) * PAIR],
                        dead,
                    )
                    for j in range(4)
                ],
                axis=1,
            )
        )
    decoded = jnp.concatenate(mixtures, axis=0)
    result = (wide(grid).astype(F32) + mm_t(decoded, weights.get(0))).astype(BF16)
    for j in range(4):
        out[j] = result[:, j * 256 : (j + 1) * 256]


def exchange(x):
    return lax.all_to_all(x, "heads", 0, 0, tiled=True)


def halo(last, first):
    size = lax.axis_size(NODES)
    up = [(i, i + 1) for i in range(size - 1)]
    down = [(j, i) for i, j in up]
    return lax.ppermute(last, NODES, up), lax.ppermute(first, NODES, down)


def after_it(x, other):
    return lax.optimization_barrier((x, other))[0]


def beside(rows):
    size = lax.axis_size(NODES)
    up = [(n * 4 + j, (n + 1) * 4 + j) for n in range(size - 1) for j in (2, 3)]
    down = [((n + 1) * 4 + j, n * 4 + j) for n in range(size - 1) for j in (0, 1)]
    return lax.ppermute(rows, (*NODES, "heads"), up + down)


def in_hbm(x):
    return pltpu.with_memory_space_constraint(x, pltpu.HBM)


def over_cores(x):
    return lax.ppermute(x, "core", [(0, 1), (1, 0)])


def trade(parts):
    out = [parts[0]]
    for k in range(1, 4):
        out.append(lax.ppermute(parts[k], "heads", [(i, i ^ k) for i in range(4)]))
    return out


def pack(sources):
    (tiles,) = call(
        pack_kernel, [(16, 20, 8, 128)], [in_vmem()] * len(sources), room=56
    )(*sources)
    return tiles


def over_plane(x):
    return lax.all_to_all(x, ("y", "x"), 0, 0, tiled=True)


def local(
    grid_state,
    mesh_state,
    encoder_query,
    encoder_key,
    encoder_value,
    encoder_output,
    window_query,
    window_key,
    window_value,
    window_output,
    expand_weight,
    shrink_weight,
    decoder_query,
    decoder_key,
    decoder_value,
    decoder_output,
    encoder_blocks,
    encoder_count,
    window_offsets,
    decoder_blocks,
    decoder_count,
):
    position = lax.axis_index(NODES)
    mesh_tiles = lax.axis_size(NODES) * 2
    pos = jnp.stack(
        [position, lax.axis_index("core"), lax.axis_index("heads"), jnp.int32(mesh_tiles),
         lax.axis_index("zh")]
    ).astype(jnp.int32)

    counts = ((1, 1, 1), (1, 1, 1, 1, 1, 4, 4, 1, 1, 1, 1))
    tiles = pack(
        (
            encoder_key, encoder_value, encoder_query, encoder_output.T, window_query, window_key,
            window_value, window_output.T, expand_weight, shrink_weight.T, decoder_key,
            decoder_value, decoder_query, decoder_output.T,
        )
    )
    tiles = lax.all_to_all(tiles, ("zh", "heads"), 0, 0, tiled=True)
    copies_a, rows = call(
        functools.partial(regroup_kernel, counts),
        [(16, 4, 8, 1536), (4, 8, 8704)],
        [in_vmem()],
    )(tiles)
    mine = lax.all_gather(rows, ("y", "x"))
    mine_a = over_plane(copies_a)
    theirs_a = over_cores(mine_a)


    head = lax.axis_index("heads")
    grid_parts, mesh_parts = grid_state.reshape(4, 256, 256), mesh_state.reshape(4, 64, 256)
    both = call(
        own_kernel, [(320, 256)], [in_smem(), in_vmem(), in_vmem()], room=8
    )(pos, grid_parts, mesh_parts)
    both += tuple(
        jnp.concatenate(
            [
                lax.dynamic_index_in_dim(after_it(x, copies_a), head ^ k, 0, False)
                for x in (grid_parts, mesh_parts)
            ]
        )
        for k in range(1, 4)
    )
    sent, grid, mesh = call(
        inputs_kernel,
        [(4, 288, 256), (4, 256, 256), (4, 64, 256)],
        [in_smem()] + [in_vmem()] * 4 + [in_any(), in_any()],
        weight_scratch(CHUNK_A, (0, 1, 2)),
        room=16,
    )(pos, *trade(both), mine_a, theirs_a)
    own = exchange(sent)
    before, after = halo(own[2:, :256], own[:2, :256])
    (sent,) = call(
        encode_kernel,
        [(4, 64, 128)],
        [in_smem()] * 3 + [in_vmem()] * 3,
        [pltpu.VMEM((16, TILE, 256), BF16), pltpu.VMEM((8 * TILE, 256), BF16)],
    )(pos, encoder_blocks, encoder_count, own, before, after)
    encoded = exchange(sent)
    mine = after_it(mine, sent)
    theirs_b = over_cores(mine[:, :, :, :2048])
    theirs = over_cores(mine)
    mine, late = in_hbm(mine), in_hbm(theirs)
    sent, kept = call(
        first_kernel,
        [(4, 64, 384), (64, D)],
        [in_smem(), in_vmem(), in_vmem(), in_any(), in_any()],
        weight_scratch(CHUNK_B, (0, 1, 2, 3)),
        room=16,
    )(pos, encoded, mesh, mine, theirs_b)
    own = exchange(sent)
    side = own[:, :, PAIR:]
    before, after = halo(side, side)
    (queries,) = call(
        queries_kernel,
        [(256, 512)],
        [in_smem(), in_vmem()] + [in_any()] * 2,
        weight_scratch(CHUNK_B, (9,)),
        room=12,
    )(pos, grid, mine, late)
    (sent,) = call(
        window_kernel,
        [(4, 64, 128)],
        [in_smem()] * 2 + [in_vmem()] * 3,
        [pltpu.VMEM((6, TILE, 256), BF16), pltpu.VMEM((4 * TILE, 256), BF16)],
    )(pos, window_offsets, own, before, after)
    windowed = exchange(sent)
    sent, spread = call(
        second_kernel,
        [(4, 64, 256), (64, D)],
        [in_smem(), in_vmem(), in_vmem()] + [in_any()] * 2,
        weight_scratch(CHUNK_B, (4, 5, 6, 7, 8)),
        room=24,
    )(pos, windowed, kept, mine, late)
    arrived = beside(spread)
    own = lax.all_gather(spread, "heads")
    sides = trade([after_it(arrived, own)] * 4)
    mesh_out = exchange(sent).reshape(256, 256)
    last = weight_scratch(CHUNK_B, (10,))
    (sent,) = call(
        decode_kernel,
        [(4, 256, 256)],
        [in_smem()] * 3 + [in_vmem()] * 7 + [in_any()] * 2,
        last[:-1]
        + [
            pltpu.VMEM((4, TILE, D), BF16),
            pltpu.VMEM((4, 64, D), BF16),
            pltpu.VMEM((3 * TILE, D), BF16),
            last[-1],
        ],
        room=16,
    )(pos, decoder_blocks, decoder_count, grid, queries, own, *sides, mine, late)
    grid_out = exchange(sent).reshape(1024, 256)
    return grid_out, mesh_out


def solution(mesh):
    sizes = (4, 4, 4, 2)
    fine = Mesh(mesh.devices.reshape(*sizes, mesh.devices.shape[1]), (*NODES, "heads"))
    both, flipped = P(NODES, "heads"), P("heads", NODES)
    in_specs = (
        both, both, both, both, both, flipped, both, both, both, flipped, both, flipped,
        both, both, both, flipped,
        P(NODES, None), P(NODES), P(NODES, None), P(NODES, None), P(NODES),
    )
    return jax.shard_map(
        local, mesh=fine, in_specs=in_specs, out_specs=(both, both), check_vma=False
    )
```
